256 devices in a mesh: blk: 64 (over x_lo, y, z), mp: 4 (over x_hi, core).
Axes of the slice: x: 4 (x_hi: 2, x_lo: 2; x = x_hi * 2 + x_lo), y: 4, z: 8, core: 2. Of those that a mesh axis runs over, the one named last changes fastest.
Arguments:
- tokens: bfloat16 [8192, 2048], P('blk', 'mp'), may hold values from -16 to 16
- grad_out: bfloat16 [8192, 2048], P('blk', 'mp'), may hold values from -0.29882812 to 0.29882812
- w_gate: bfloat16 [2048, 2560], P(None, 'mp'), may hold values from -0.125 to 0.125
- w_lin: bfloat16 [2048, 2560], P(None, 'mp'), may hold values from -0.125 to 0.125
- w_out_t: bfloat16 [2048, 2560], P(None, 'mp'), may hold values from -0.125 to 0.125
- code: float32 [64, 5], P('blk'), may hold values from 0.5 to 2
- decode: float32 [64], P('blk'), may hold values from 0.05 to 0.2
- stragglers: int32 [4], replicated, may hold values from 0 to 63, as said below
Outputs:
- grads: float32 [2048, 3, 2560], P('blk', None, 'mp')
The draws below stay inside these ranges and needn't reach their ends.
Inputs may be any that keep to these rules, and one draw needn't show every extreme that they name: `stragglers`: 4 distinct worker indices; worker 0 and worker 64 - 1 are always among them.
All inputs are finite; a program needn't handle non-finite values.
Results may differ from the reference program's by a relative error of at most 0.0042.
Values may be sent and summed in bfloat16 or wider, within the bound.
No kernel may reach another device: no remote copies, remote signals or barrier semaphores. Data moves between devices by JAX's collectives and lax.ppermute only.
A program may use at most 128 MiB of HBM per device.

```python
import math
from functools import partial
import jax
import jax.numpy as jnp
from jax import lax

D = 2048
FF = 2560
S1 = 5
NSTRAG = 4
R = 128
TOKENS = 8192
N_BLK = 64


def draw_stragglers(key, part):
    order = jax.random.permutation(key, jnp.arange(N_BLK - 2, dtype=jnp.int32)) + 1
    ends = jnp.array([0, N_BLK - 1], dtype=jnp.int32)
    return jnp.concatenate([ends, order[:NSTRAG - 2]]).astype(jnp.int32)


def spiked(drawn, key, source, target, parts, factor):
    owner, partner = [(jnp.arange(drawn.shape[dim]) // (drawn.shape[dim] // parts)).reshape([-1 if axis == dim else 1 for axis in range(drawn.ndim)]) for dim in (source, target)]
    chosen = jax.random.permutation(key, parts)[partner]
    strong = (owner == chosen) | (owner == (partner + parts // 2) % parts)
    return jnp.where(strong, factor * drawn, drawn)


def level_of(key, dims, cuts, low, high):
    factor_of, own = 1.0, jax.random.fold_in(key, 6)
    for dim, shards_of in cuts:
        heights = jnp.exp(jax.random.uniform(jax.random.fold_in(own, dim), (shards_of,), jnp.float32, low / len(cuts), high / len(cuts)))
        factor_of = factor_of * jnp.repeat(heights, dims[dim] // shards_of).reshape([-1 if axis == dim else 1 for axis in range(len(dims))])
    return factor_of


def scatter_about(key, shape, width, reach, split=(), held_as=jnp.bfloat16):
    result = width * jax.random.normal(key, shape, jnp.float32)
    if split:
        result = result * level_of(key, shape, split, -0.22, 0.18)
    return jnp.clip(result, -reach, reach).astype(held_as)


def bell_draw_with(own_key, shape, deviation, limit, split, heavy, held_as=jnp.bfloat16):
    result = deviation * jax.random.normal(own_key, shape, jnp.float32)
    if split:
        result = result * level_of(own_key, shape, split, -0.22, 0.18)
    return jnp.clip(spiked(result, jax.random.fold_in(own_key, 3), *heavy), -limit, limit).astype(held_as)


def setup_inputs(seed: int = 0) -> dict:
    key_of = jax.random.split(jax.random.key(seed), 9)
    tokens = bell_draw_with(key_of[0], (TOKENS, D), 1.0, 16.0, ((0, 64), (1, 4)), (0, 1, 64, 4.0))
    grad_out = scatter_about(key_of[1], (TOKENS, D), 0.05, 0.29882812, ((0, 64), (1, 4)))
    w_gate = scatter_about(key_of[2], (D, FF), D ** -0.5, 0.125, ((1, 4),))
    w_lin = scatter_about(key_of[3], (D, FF), D ** -0.5, 0.125, ((1, 4),))
    w_out_t = scatter_about(key_of[4], (D, FF), FF ** -0.5, 0.125, ((1, 4),))
    code = jnp.clip(jnp.exp(math.log(2.0) - 1.3862944 * jax.random.uniform(key_of[5], (N_BLK, S1), jnp.float32) ** level_of(key_of[5], (N_BLK, S1), ((0, 64),), -0.2, 0.2)), 0.5, 2.0)
    decode = jnp.clip(jnp.exp(math.log(0.2) - 1.3862944 * jax.random.uniform(key_of[6], (N_BLK,), jnp.float32) ** level_of(key_of[6], (N_BLK,), ((0, 64),), -0.2, 0.2)), 0.05, 0.2)
    stragglers = draw_stragglers(jax.random.fold_in(key_of[8], 71), 0)
    return {"tokens": tokens, "grad_out": grad_out, "w_gate": w_gate, "w_lin": w_lin, "w_out_t": w_out_t, "code": code, "decode": decode, "stragglers": stragglers}


def local_grads(inputs, cotangent, w_gate, w_lin, w_out_t):
    gate_pre = jnp.dot(inputs, w_gate, preferred_element_type=jnp.float32)
    linear = jnp.dot(inputs, w_lin, preferred_element_type=jnp.float32)
    activated, pullback = jax.vjp(partial(jax.nn.gelu, approximate=True), gate_pre)
    hidden = (activated * linear).astype(jnp.bfloat16)
    hidden_grad = jnp.dot(cotangent, w_out_t, preferred_element_type=jnp.float32)
    d_gate = pullback(hidden_grad * linear)[0].astype(jnp.bfloat16)
    d_lin = (hidden_grad * activated).astype(jnp.bfloat16)
    return (jnp.concatenate([d_gate, d_lin], axis=1), hidden)

def reference(tokens, grad_out, w_gate, w_lin, w_out_t, code, decode, stragglers):
    worker_ids = jnp.arange(N_BLK, dtype=jnp.int32)
    is_alive = jnp.all(worker_ids[:, None] != stragglers[None, :], axis=1)
    own_decode = jnp.where(is_alive, decode, jnp.float32(0.0)).astype(jnp.float32)
    slot_ids = jnp.arange(S1, dtype=jnp.int32)
    owners = ((worker_ids[:, None] - slot_ids[None, :]) % N_BLK).astype(jnp.int32)
    slot_grid = jnp.broadcast_to(slot_ids[None, :], owners.shape)
    partition_weight = lax.optimization_barrier(jnp.sum(own_decode[owners] * code[owners, slot_grid], axis=1)).astype(jnp.float32)
    inputs = tokens.reshape(N_BLK, R, D)
    cotangents = grad_out.reshape(N_BLK, R, D)

    def accumulate(accum, items):
        inputs_p, cotangent_p, weight_p = items
        right_side, hidden = local_grads(inputs_p, cotangent_p, w_gate, w_lin, w_out_t)
        product = jnp.concatenate([jnp.dot(inputs_p.T, right_side, preferred_element_type=jnp.float32), jnp.dot(cotangent_p.T, hidden, preferred_element_type=jnp.float32)], axis=1)
        return (accum + weight_p * product, None)
    start_value = jnp.zeros((D, 3 * FF), jnp.float32)
    accum = lax.scan(accumulate, start_value, (inputs, cotangents, partition_weight))[0]
    return accum.reshape(D, 3, FF)
```

```python
import jax
import jax.numpy as jnp
from jax import lax
from jax.experimental import pallas as pl
from jax.experimental.pallas import tpu as pltpu
from jax.sharding import Mesh, PartitionSpec as P

BF16 = jnp.bfloat16
F32 = jnp.float32
ROOT_2_PI = 0.7978845608028654
CUBIC = 0.044715
NX, NY, NZ = 4, 4, 8


def swapped(block, axis, size, flip):
    return lax.ppermute(block, axis, [(i, i ^ flip) for i in range(size)])


def along_x(block, flip):
    return swapped(block, ("xl", "xh"), NX, 2 * (flip & 1) + (flip >> 1))


def along_y(block, flip):
    return swapped(block, "y", NY, flip)


def sibling(block):
    return swapped(block, "c", 2, 1)


def along_z(block, step):
    return lax.ppermute(block, "z", [(i, (i + step) % NZ) for i in range(NZ)])


def kernel(index, weight, *refs):
    tokens, grads = refs[0:8], refs[8:16]
    w_gate, w_lin, w_out = refs[16:19]
    out = refs[19]
    dh, gates, hidden = refs[20:23]
    shards = [index[i] for i in range(4)]
    half = index[4]
    offset = index[5]

    def product(blocks, weights):
        total = None
        for i, block in enumerate(blocks):
            part = jnp.dot(block, weights[shards[i]], preferred_element_type=F32)
            total = part if total is None else total + part
        return total

    for ex in range(2):
        blocks = [grads[eh * 2 + ex + 4 * ec][...].reshape(512, 512) for eh in range(2) for ec in range(2)]
        dh[ex] = product(blocks, w_out).reshape(4, 128, 640)

    for dy in range(4):
        blocks = [tokens[dy + 4 * ec][2 * eh : 2 * eh + 2].reshape(256, 512) for eh in range(2) for ec in range(2)]
        pre = product(blocks, w_gate)
        lin = product(blocks, w_lin)
        for ex in range(2):
            u = pre[128 * ex : 128 * ex + 128]
            v = lin[128 * ex : 128 * ex + 128]
            w = weight[dy * 2 + ex]
            square = u * u
            t = jnp.tanh(ROOT_2_PI * (u + CUBIC * (square * u)))
            cdf = 0.5 * (1.0 + t)
            act = u * cdf
            slope = cdf + 0.5 * u * (1.0 - t * t) * (ROOT_2_PI * (1.0 + 3.0 * CUBIC * square))
            d = dh[ex, dy] * w
            rows = pl.ds(dy * 256 + ex * 128, 128)
            gates[rows, 0:640] = (d * v * slope).astype(BF16)
            gates[rows, 640:1280] = (d * act).astype(BF16)
            hidden[rows, :] = (act * v * w).astype(BF16)

    def columns(first, second):
        own = jnp.where(half == 0, first, second)
        return jnp.where(offset == 0, own[:, 0:256], own[:, 256:512])

    eh = index[6]
    xs = jnp.concatenate(
        [columns(tokens[dy][pl.ds(2 * eh, 2)].reshape(256, 512), tokens[dy + 4][pl.ds(2 * eh, 2)].reshape(256, 512)) for dy in range(4)], axis=0
    )
    ys = []
    for dy in range(4):
        for ex in range(2):
            near = jnp.where(eh == 0, grads[ex][dy], grads[2 + ex][dy])
            far = jnp.where(eh == 0, grads[4 + ex][dy], grads[6 + ex][dy])
            ys.append(columns(near, far))
    ys = jnp.concatenate(ys, axis=0)
    dims = (((0,), (0,)), ((), ()))
    out[:, 0:1280] = lax.dot_general(xs, gates[...], dims, preferred_element_type=F32)
    out[:, 1280:1920] = lax.dot_general(ys, hidden[...], dims, preferred_element_type=F32)


def plane_grads(index, weight, tokens, grads, w_gate, w_lin, w_out):
    smem = pl.BlockSpec(memory_space=pltpu.SMEM)
    vmem = pl.BlockSpec(memory_space=pltpu.VMEM)
    return pl.pallas_call(
        kernel,
        out_shape=jax.ShapeDtypeStruct((256, 1920), F32),
        in_specs=[smem, smem] + [vmem] * 19,
        out_specs=vmem,
        scratch_shapes=[
            pltpu.VMEM((2, 4, 128, 640), F32),
            pltpu.VMEM((1024, 1280), BF16),
            pltpu.VMEM((1024, 640), BF16),
        ],
        compiler_params=pltpu.CompilerParams(vmem_limit_bytes=56 * 1024 * 1024),
        name="plane_grads",
    )(index, weight, *tokens, *grads, w_gate, w_lin, w_out)


def plane_weights(code, decode, stragglers, xl, y, z):
    device = (xl * NY + y) * NZ + z
    alive = jnp.all(stragglers != device)
    row = jnp.where(alive, decode[0], F32(0.0)) * code[0]
    workers = jnp.arange(64, dtype=jnp.int32)
    slot = (workers - z) % NZ
    picked = jnp.where(slot < 5, 1.0, 0.0) * sum(jnp.where(slot == j, row[j], 0.0) for j in range(5))
    values = lax.all_to_all(picked.reshape(64, 1), ("xl", "y", "z"), 0, 0, tiled=True).reshape(64)
    totals = sum(jnp.roll(values, j) for j in range(5))
    wanted = jnp.stack([((xl ^ ex) * NY + (y ^ dy)) * NZ + z for dy in range(4) for ex in range(2)])
    return jnp.sum(jnp.where(wanted[:, None] == workers[None, :], totals[None, :], 0.0), axis=1)


def summed_over_z(partial, z):
    parts = partial.reshape(NZ, 32, 1920)

    def own(k):
        return lax.dynamic_index_in_dim(parts, (z + k) % NZ, 0, keepdims=False)

    cut = 1024
    up = along_z(own(4)[:, :cut].astype(BF16), 1).astype(F32)
    down = along_z(own(-4)[:, cut:].astype(BF16), -1).astype(F32)
    up = jnp.concatenate([up + own(3)[:, :cut], own(3)[:, cut:]], axis=1).astype(BF16)
    down = jnp.concatenate([own(-3)[:, :cut], down + own(-3)[:, cut:]], axis=1).astype(BF16)
    for k in (2, 1, 0):
        up = along_z(up, 1).astype(F32)
        down = along_z(down, -1).astype(F32)
        if k:
            up = (up + own(k)).astype(BF16)
            down = (down + own(-k)).astype(BF16)
    return own(0) + up + down


def shards(tokens, grad_out, w_gate, w_lin, w_out_t, code, decode, stragglers):
    xl, y, z, xh, c = (lax.axis_index(a).astype(jnp.int32) for a in ("xl", "y", "z", "xh", "c"))
    tokens_row = jnp.stack([tokens] + [along_x(tokens, k) for k in (1, 2, 3)])
    grads_row = jnp.stack([grad_out] + [along_y(grad_out, k) for k in (1, 2, 3)])
    weight = plane_weights(code, decode, stragglers, xl, y, z)
    tokens_all = [tokens_row] + [along_y(tokens_row, k) for k in (1, 2, 3)]
    grads_all = [grads_row] + [along_x(grads_row, k) for k in (1, 2, 3)]
    tokens_all += [sibling(block) for block in tokens_all]
    grads_all += [sibling(block) for block in grads_all]
    index = jnp.stack(
        [(xh ^ eh) * 2 + (c ^ ec) for eh in range(2) for ec in range(2)] + [(y >> 1) ^ c, y & 1, xl ^ xh]
    )
    weights = [w.reshape(4, 512, 640) for w in (w_gate, w_lin, w_out_t)]
    partial = plane_grads(index, weight, tokens_all, grads_all, *weights)
    return summed_over_z(partial, z).reshape(32, 3, 640)


def solution(mesh):
    split = Mesh(mesh.devices.reshape(2, NY, NZ, 2, 2), ("xl", "y", "z", "xh", "c"))
    blk, mp = ("xl", "y", "z"), ("xh", "c")
    in_specs = (P(blk, mp), P(blk, mp), P(None, mp), P(None, mp), P(None, mp), P(blk, None), P(blk), P())
    return jax.shard_map(shards, mesh=split, in_specs=in_specs, out_specs=P(blk, None, mp), check_vma=False)
```

```python
import jax
import jax.numpy as jnp
from jax import lax
from jax.experimental import pallas as pl
from jax.experimental.pallas import tpu as pltpu
from jax.sharding import Mesh, PartitionSpec as P


BF16 = jnp.bfloat16
F32 = jnp.float32
I32 = jnp.int32
ROOT_2_PI = 0.7978845608028654
CUBIC = 0.044715
BLK = ("xl", "y", "z")
PLANE = ("xl", "y", "xh", "c")
SMEM = pl.BlockSpec(memory_space=pltpu.SMEM)
VMEM = pl.BlockSpec(memory_space=pltpu.VMEM)
PARAMS = pltpu.CompilerParams(vmem_limit_bytes=16 * 1024 * 1024)


def place():
    return [lax.axis_index(a).astype(I32) for a in ("xl", "y", "z", "xh", "c")]


def across(block, flip, first):
    route = []
    for xl in range(2):
        for y in range(4):
            for xh in range(2):
                for c in range(2):
                    on_x = (c == 0) == first
                    to = (xl ^ (flip & 1), y, xh ^ (flip >> 1), c) if on_x else (xl, y ^ flip, xh, c)
                    number = lambda a: ((a[0] * 4 + a[1]) * 2 + a[2]) * 2 + a[3]
                    route.append((number((xl, y, xh, c)), number(to)))
    return lax.ppermute(block, PLANE, route)


def sibling(block):
    return lax.ppermute(block, "c", [(0, 1), (1, 0)])


def partner_of(z, c):
    return z ^ 1 if c == 0 else ((z + 1) % 8 if z % 2 else (z - 1) % 8)


def z_pair(block):
    return lax.ppermute(block, ("z", "c"), [(z * 2 + c, partner_of(z, c) * 2 + c) for z in range(8) for c in range(2)])


def z_step(block, step):
    return lax.ppermute(block, "z", [(z, (z + step) % 8) for z in range(8)])


def prepare_kernel(code, decode, stragglers, w_gate, w_lin, w_out_t, picked, w_in, w_out, sems):
    copies = [
        pltpu.make_async_copy(w_gate, w_in.at[:, :, pl.ds(0, 640)], sems.at[0]),
        pltpu.make_async_copy(w_lin, w_in.at[:, :, pl.ds(640, 640)], sems.at[1]),
        pltpu.make_async_copy(w_out_t, w_out, sems.at[2]),
    ]
    for copy in copies:
        copy.start()
    xl, y, z, _, _ = place()
    device = (xl * 4 + y) * 8 + z
    alive = stragglers[0] != device
    for i in range(1, 4):
        alive = alive & (stragglers[i] != device)
    scale = jnp.where(alive, decode[0], 0.0)
    slot = (lax.broadcasted_iota(I32, (64, 128), 0) - z) & 7
    value = jnp.zeros((64, 128), F32)
    for j in range(5):
        value = jnp.where(slot == j, scale * code[0, j], value)
    picked[...] = value
    for copy in copies:
        copy.wait()


def prepare(code, decode, stragglers, w_gate, w_lin, w_out_t):
    whole = pl.BlockSpec(memory_space=pltpu.HBM)
    return pl.pallas_call(
        prepare_kernel,
        out_shape=(
            jax.ShapeDtypeStruct((64, 128), F32),
            jax.ShapeDtypeStruct((4, 512, 1280), BF16),
            jax.ShapeDtypeStruct((4, 512, 640), BF16),
        ),
        in_specs=[SMEM] * 3 + [whole] * 3,
        out_specs=(VMEM, VMEM, VMEM),
        scratch_shapes=[pltpu.SemaphoreType.DMA((3,))],
        compiler_params=PARAMS,
        name="prepare",
    )(code, decode, stragglers, *[w.reshape(4, 512, 640) for w in (w_gate, w_lin, w_out_t)])


def first_kernel(own, other, w_in, w_out, acc, cols):
    acc[...] = jnp.zeros_like(acc)
    gather_kernel(0, own, other, w_in, w_out, acc, cols)


def middle_kernel(m, own, other, w_in, w_out, _, __, acc, cols):
    gather_kernel(m, own, other, w_in, w_out, acc, cols)


def final_kernel(m, own, other, w_in, w_out, _, __, values, acc, cols, *rest):
    gather_kernel(m, own, other, w_in, w_out, acc, cols)
    last_kernel(values, acc, cols, *rest)


def gather_kernel(m, own, other, w_in, w_out, acc, cols):
    xl, y, _, xh, c = place()
    for ec, block in ((0, own), (1, other)):
        x_first = (c ^ ec) == 0

        def step(j, _):
            eh = jnp.where(x_first, j, m >> 1)
            p0 = jnp.where(x_first, 2 * m, 4 * j + (m & 1))
            p1 = jnp.where(x_first, 2 * m + 1, 4 * j + 2 + (m & 1))
            shard = (xh ^ eh) * 2 + (c ^ ec)
            xs = block[pl.ds(2 * j, 2), 0].reshape(256, 512)
            ys = block[pl.ds(2 * j, 2), 1].reshape(256, 512)
            pre = jnp.dot(xs, w_in[shard], preferred_element_type=F32)
            acc[0, p0] += pre[:128, :640]
            acc[1, p0] += pre[:128, 640:]
            acc[0, p1] += pre[128:, :640]
            acc[1, p1] += pre[128:, 640:]
            dh = jnp.dot(ys, w_out[shard], preferred_element_type=F32)
            acc[2, p0] += dh[:128]
            acc[2, p1] += dh[128:]

            @pl.when((ec == ((y >> 1) ^ c)) & (eh == (xl ^ xh)))
            def _():
                low = (y & 1) == 0
                for n, v in ((0, xs), (1, ys)):
                    v = jnp.where(low, v[:, :256], v[:, 256:])
                    cols[n, p0] = v[:128]
                    cols[n, p1] = v[128:]

            return 0

        lax.fori_loop(0, 2, step, 0)


STATE = (jax.ShapeDtypeStruct((3, 8, 128, 640), F32), jax.ShapeDtypeStruct((2, 8, 128, 256), BF16))


def priced(giga):
    return pl.CostEstimate(flops=giga << 30, bytes_accessed=1 << 20, transcendentals=0)


def gathered(m, own, other, w_in, w_out, state):
    return pl.pallas_call(
        (lambda *refs: middle_kernel(m, *refs)) if state else first_kernel,
        out_shape=STATE,
        in_specs=[VMEM] * (4 + len(state)),
        out_specs=(VMEM, VMEM),
        input_output_aliases={4: 0, 5: 1} if state else {},
        compiler_params=PARAMS,
        cost_estimate=priced(2),
    )(own, other, w_in, w_out, *state)


def finished(m, own, other, w_in, w_out, state, values):
    return pl.pallas_call(
        lambda *refs: final_kernel(m, *refs),
        out_shape=STATE
        + (jax.ShapeDtypeStruct((4, 3, 32, 640), F32), jax.ShapeDtypeStruct((4, 3, 32, 640), BF16)),
        in_specs=[VMEM] * 7,
        out_specs=(VMEM,) * 4,
        input_output_aliases={4: 0, 5: 1},
        scratch_shapes=[
            pltpu.VMEM((8, 128, 1280), BF16),
            pltpu.VMEM((8, 128, 640), BF16),
            pltpu.VMEM((8, 3, 32, 640), F32),
        ],
        compiler_params=PARAMS,
        cost_estimate=priced(4),
        name="finish",
    )(own, other, w_in, w_out, *state, values)[2:]


def last_kernel(values, acc, cols, keep, send, gates, hidden, total):
    xl, y, z, _, c = place()
    workers = lax.broadcasted_iota(I32, (64, 128), 0)

    def part(p, _):
        dy, ex = p >> 1, p & 1
        number = ((xl ^ ex) * 4 + (y ^ dy)) * 8 + z
        mask = ((number - workers) & 63) < 5
        w = jnp.sum(jnp.where(mask, values[...], 0.0), axis=0, keepdims=True)[:, :1]
        for r in range(0, 128, 32):
            rows = pl.ds(r, 32)
            u = acc[0, p, rows]
            v = acc[1, p, rows]
            d = acc[2, p, rows] * w
            square = u * u
            t = jnp.tanh(ROOT_2_PI * (u + CUBIC * (square * u)))
            cdf = 0.5 * (1.0 + t)
            act = u * cdf
            slope = cdf + 0.5 * u * (1.0 - t * t) * (ROOT_2_PI * (1.0 + 3.0 * CUBIC * square))
            gates[p, rows, 0:640] = (d * v * slope).astype(BF16)
            gates[p, rows, 640:1280] = (d * act).astype(BF16)
            hidden[p, rows] = (act * v * w).astype(BF16)
        return 0

    lax.fori_loop(0, 8, part, 0)
    dims = (((0,), (0,)), ((), ()))
    both = lax.dot_general(
        cols[0].reshape(1024, 256), gates[...].reshape(1024, 1280), dims, preferred_element_type=F32
    )
    total[:, 0] = both[:, :640].reshape(8, 32, 640)
    total[:, 1] = both[:, 640:].reshape(8, 32, 640)
    total[:, 2] = lax.dot_general(
        cols[1].reshape(1024, 256), hidden[...].reshape(1024, 640), dims, preferred_element_type=F32
    ).reshape(8, 32, 640)
    odd = z & 1
    near = jnp.where(odd == 1, z + 1, z - 1) & 7
    near = jnp.where(c == 0, z ^ 1, near)
    for k in range(4):
        keep[k] = total[((z >> 1) + k & 3) * 2 + odd]
        send[k] = total[((near >> 1) + k & 3) * 2 + (1 - odd)].astype(BF16)


def all_steps(tokens, grad_out, w_gate, w_lin, w_out_t, code, decode, stragglers):
    own = jnp.stack([tokens, grad_out])
    row = [own] + [across(own, k, True) for k in (1, 2, 3)]
    picked, w_in, w_out = prepare(code, decode, stragglers, w_gate, w_lin, w_out_t)
    row, picked = lax.optimization_barrier((jnp.stack(row), picked))
    near = [row]
    for k in (1, 2, 3):
        near.append(across(row, k, False))
    values = lax.all_to_all(picked, BLK, 0, 0, tiled=True)
    swap = sibling(row)
    first, values = lax.optimization_barrier((row, values))
    state = gathered(0, first, swap, w_in, w_out, ())
    state, near[1], near[3] = lax.optimization_barrier((state, near[1], near[3]))
    other = {k: sibling(near[k]) for k in (1, 3)}
    for m in (1, 3):
        state = gathered(m, near[m], other[m], w_in, w_out, state)
    state, near[2] = lax.optimization_barrier((state, near[2]))
    keep, send = finished(2, near[2], sibling(near[2]), w_in, w_out, state, values)
    got = z_pair(send)
    mixed = keep + got.astype(F32)
    result = mixed[0]
    for k in (1, 3, 2):
        result = result + z_step(mixed[k].astype(BF16), 2 * k).astype(F32)
    return jnp.transpose(result, (1, 0, 2))


def solution(mesh):
    split = Mesh(mesh.devices.reshape(2, 4, 8, 2, 2), ("xl", "y", "z", "xh", "c"))
    mp = ("xh", "c")
    in_specs = (P(BLK, mp), P(BLK, mp), P(None, mp), P(None, mp), P(None, mp), P(BLK, None), P(BLK), P())
    return jax.shard_map(all_steps, mesh=split, in_specs=in_specs, out_specs=P(BLK, None, mp), check_vma=False)
```

```python
import jax
import jax.numpy as jnp
from jax import lax
from jax.experimental import pallas as pl
from jax.experimental.pallas import tpu as pltpu
from jax.sharding import Mesh, PartitionSpec as P


BF16 = jnp.bfloat16
F32 = jnp.float32
I32 = jnp.int32
ROOT_2_PI = 0.7978845608028654
CUBIC = 0.044715
BLK = ("xl", "y", "z")
PLANE = ("xl", "y", "xh", "c")
SMEM = pl.BlockSpec(memory_space=pltpu.SMEM)
VMEM = pl.BlockSpec(memory_space=pltpu.VMEM)
PARAMS = pltpu.CompilerParams(vmem_limit_bytes=16 * 1024 * 1024)


def place():
    return [lax.axis_index(a).astype(I32) for a in ("xl", "y", "z", "xh", "c")]


def across(block, flip, first):
    route = []
    for xl in range(2):
        for y in range(4):
            for xh in range(2):
                for c in range(2):
                    on_x = (c == 0) == first
                    to = (xl ^ (flip & 1), y, xh ^ (flip >> 1), c) if on_x else (xl, y ^ flip, xh, c)
                    number = lambda a: ((a[0] * 4 + a[1]) * 2 + a[2]) * 2 + a[3]
                    route.append((number((xl, y, xh, c)), number(to)))
    return lax.ppermute(block, PLANE, route)


def sibling(block):
    return lax.ppermute(block, "c", [(0, 1), (1, 0)])


def partner_of(z, c):
    return z ^ 1 if c == 0 else ((z + 1) % 8 if z % 2 else (z - 1) % 8)


def z_pair(block):
    return lax.ppermute(block, ("z", "c"), [(z * 2 + c, partner_of(z, c) * 2 + c) for z in range(8) for c in range(2)])


def z_step(block, step):
    return lax.ppermute(block, "z", [(z, (z + step) % 8) for z in range(8)])


def hbm(array):
    return pltpu.with_memory_space_constraint(array, pltpu.HBM)


def message_kernel(decode, code_in, stragglers_in, tokens, grad_out, out, code, stragglers, sems):
    pairs = (
        (tokens, out.at[pl.ds(0, 128)]),
        (grad_out, out.at[pl.ds(128, 128)]),
        (code_in, code),
        (stragglers_in, stragglers),
    )
    copies = [pltpu.make_async_copy(source, target, sems.at[i]) for i, (source, target) in enumerate(pairs)]
    for copy in copies:
        copy.start()
    for copy in copies[2:]:
        copy.wait()
    xl, y, z, _, _ = place()
    device = (xl * 4 + y) * 8 + z
    alive = stragglers[0] != device
    for i in range(1, 4):
        alive = alive & (stragglers[i] != device)
    scale = jnp.where(alive, decode[0], 0.0)
    lane = lax.broadcasted_iota(I32, (8, 128), 1)
    row = lax.broadcasted_iota(I32, (8, 128), 0)
    value = jnp.zeros((8, 128), F32)
    for j in range(5):
        value = jnp.where(lane == j, scale * code[0, j], value)
    high = value.astype(BF16).astype(F32)
    rest = value - high
    middle = rest.astype(BF16).astype(F32)
    low = rest - middle
    pieces = jnp.where(row == 0, high, jnp.where(row == 1, middle, jnp.where(row == 2, low, 0.0)))
    out[256:264, :] = jnp.zeros((8, 512), BF16)
    out[256:264, 0:128] = pieces.astype(BF16)
    for copy in copies[:2]:
        copy.wait()


def message(code, decode, stragglers, tokens, grad_out):
    return pl.pallas_call(
        message_kernel,
        out_shape=jax.ShapeDtypeStruct((264, 512), BF16),
        in_specs=[SMEM] + [pl.BlockSpec(memory_space=pltpu.HBM)] * 4,
        out_specs=VMEM,
        scratch_shapes=[pltpu.SMEM((1, 5), F32), pltpu.SMEM((4,), I32), pltpu.SemaphoreType.DMA((4,))],
        compiler_params=PARAMS,
        name="message",
    )(decode, *[hbm(a) for a in (code, stragglers, tokens, grad_out)])


def weights_kernel(w_gate, w_lin, w_out_t, w_in, w_out, token, sems):
    copies = [
        pltpu.make_async_copy(w_gate, w_in.at[:, :, pl.ds(0, 640)], sems.at[0]),
        pltpu.make_async_copy(w_lin, w_in.at[:, :, pl.ds(640, 640)], sems.at[1]),
        pltpu.make_async_copy(w_out_t, w_out, sems.at[2]),
    ]
    for copy in copies:
        copy.start()
    token[...] = jnp.zeros_like(token)
    for copy in copies:
        copy.wait()


def loaded_weights(w_gate, w_lin, w_out_t):
    return pl.pallas_call(
        weights_kernel,
        out_shape=(
            jax.ShapeDtypeStruct((4, 512, 1280), BF16),
            jax.ShapeDtypeStruct((4, 512, 640), BF16),
            jax.ShapeDtypeStruct((8, 128), F32),
        ),
        in_specs=[pl.BlockSpec(memory_space=pltpu.HBM)] * 3,
        out_specs=(VMEM, VMEM, VMEM),
        scratch_shapes=[pltpu.SemaphoreType.DMA((3,))],
        compiler_params=PARAMS,
        name="load",
    )(*[hbm(w.reshape(4, 512, 640)) for w in (w_gate, w_lin, w_out_t)])


def read_rows(ex, own, other, rows):
    c = lax.axis_index("c").astype(I32)
    for dy in range(4):
        piece = [block[dy, 256:264, 0:128].astype(F32) for block in (own, other)]
        piece = jnp.where(c == 1, piece[0], piece[1])
        rows[2 * dy + ex : 2 * dy + ex + 1, :] = jnp.sum(piece, axis=0, keepdims=True)


def first_kernel(own, other, w_in, w_out, acc, cols, rows):
    acc[...] = jnp.zeros_like(acc)
    rows[...] = jnp.zeros_like(rows)
    read_rows(0, own, other, rows)
    gather_kernel(0, ((0, own), (1, other)), w_in, w_out, acc, cols)


def second_kernel(own, other, w_in, w_out, _, __, ___, acc, cols, rows):
    rows[...] = ___[...]
    read_rows(1, own, other, rows)
    gather_kernel(1, ((0, own), (1, other)), w_in, w_out, acc, cols)


def middle_kernel(m, *refs):
    *blocks, w_in, w_out, _, __, acc, cols = refs
    gather_kernel(m, tuple(enumerate(blocks)), w_in, w_out, acc, cols)


def final_kernel(m, other, w_in, w_out, _, __, *refs):
    rows, (acc, cols, *rest) = refs[:5], refs[5:]
    gather_kernel(m, ((1, other),), w_in, w_out, acc, cols)
    last_kernel(rows, acc, cols, *rest)


def gather_kernel(m, blocks, w_in, w_out, acc, cols):
    xl, y, _, xh, c = place()
    for ec, block in blocks:
        x_first = (c ^ ec) == 0

        def step(j, _):
            eh = jnp.where(x_first, j, m >> 1)
            p0 = jnp.where(x_first, 2 * m, 4 * j + (m & 1))
            p1 = jnp.where(x_first, 2 * m + 1, 4 * j + 2 + (m & 1))
            shard = (xh ^ eh) * 2 + (c ^ ec)
            xs = block[pl.ds(2 * j, 2), 0:128].reshape(256, 512)
            ys = block[pl.ds(2 * j, 2), 128:256].reshape(256, 512)
            pre = jnp.dot(xs, w_in[shard], preferred_element_type=F32)
            acc[0, p0] += pre[:128, :640]
            acc[1, p0] += pre[:128, 640:]
            acc[0, p1] += pre[128:, :640]
            acc[1, p1] += pre[128:, 640:]
            dh = jnp.dot(ys, w_out[shard], preferred_element_type=F32)
            acc[2, p0] += dh[:128]
            acc[2, p1] += dh[128:]

            @pl.when((ec == ((y >> 1) ^ c)) & (eh == (xl ^ xh)))
            def _():
                low = (y & 1) == 0
                for n, v in ((0, xs), (1, ys)):
                    v = jnp.where(low, v[:, :256], v[:, 256:])
                    cols[n, p0] = v[:128]
                    cols[n, p1] = v[128:]

            return 0

        lax.fori_loop(0, 2, step, 0)


STATE = (jax.ShapeDtypeStruct((3, 8, 128, 640), F32), jax.ShapeDtypeStruct((2, 8, 128, 256), BF16))


def priced(giga):
    return pl.CostEstimate(flops=giga << 30, bytes_accessed=1 << 20, transcendentals=0)


ROWS = jax.ShapeDtypeStruct((8, 128), F32)


def gathered(m, blocks, w_in, w_out, state):
    n = len(blocks) + 2
    with_rows = m in (0, 1)
    kernels = {0: first_kernel, 1: second_kernel}
    return pl.pallas_call(
        kernels.get(m, lambda *refs: middle_kernel(m, *refs)),
        out_shape=STATE + ((ROWS,) if with_rows else ()),
        in_specs=[VMEM] * (n + len(state)),
        out_specs=(VMEM,) * (3 if with_rows else 2),
        input_output_aliases={n: 0, n + 1: 1} if state else {},
        compiler_params=PARAMS,
        cost_estimate=priced(len(blocks)),
    )(*blocks, w_in, w_out, *state)


def finished(m, other, w_in, w_out, state, rows):
    return pl.pallas_call(
        lambda *refs: final_kernel(m, *refs),
        out_shape=STATE
        + (jax.ShapeDtypeStruct((4, 3, 32, 640), F32), jax.ShapeDtypeStruct((4, 3, 32, 640), BF16)),
        in_specs=[VMEM] * 10,
        out_specs=(VMEM,) * 4,
        input_output_aliases={3: 0, 4: 1},
        scratch_shapes=[
            pltpu.VMEM((8, 128, 1280), BF16),
            pltpu.VMEM((8, 128, 640), BF16),
            pltpu.VMEM((8, 3, 32, 640), F32),
        ],
        compiler_params=PARAMS,
        cost_estimate=priced(4),
        name="finish",
    )(other, w_in, w_out, *state, *rows)[2:]


def last_kernel(rows, acc, cols, keep, send, gates, hidden, total):
    xl, y, z, _, c = place()
    lane = lax.broadcasted_iota(I32, (8, 128), 1)
    line = lax.broadcasted_iota(I32, (8, 128), 0)
    line = (xl ^ (line & 1)) * 4 + (y ^ (line >> 1))
    worker = line * 8 + ((z - lane) & 7)
    terms = jnp.zeros((8, 128), F32)
    for j in range(5):
        terms = jnp.where(lane == j, rows[j][...], terms)

    def part(p, _):
        dy, ex = p >> 1, p & 1
        number = ((xl ^ ex) * 4 + (y ^ dy)) * 8 + z
        mine = (((number - lane) & 63) == worker) & (lane < 5)
        w = jnp.sum(jnp.where(mine, terms, 0.0))
        for r in range(0, 128, 32):
            rows = pl.ds(r, 32)
            u = acc[0, p, rows]
            v = acc[1, p, rows]
            d = acc[2, p, rows] * w
            square = u * u
            t = jnp.tanh(ROOT_2_PI * (u + CUBIC * (square * u)))
            cdf = 0.5 * (1.0 + t)
            act = u * cdf
            slope = cdf + 0.5 * u * (1.0 - t * t) * (ROOT_2_PI * (1.0 + 3.0 * CUBIC * square))
            gates[p, rows, 0:640] = (d * v * slope).astype(BF16)
            gates[p, rows, 640:1280] = (d * act).astype(BF16)
            hidden[p, rows] = (act * v * w).astype(BF16)
        return 0

    lax.fori_loop(0, 8, part, 0)
    dims = (((0,), (0,)), ((), ()))
    both = lax.dot_general(
        cols[0].reshape(1024, 256), gates[...].reshape(1024, 1280), dims, preferred_element_type=F32
    )
    total[:, 0] = both[:, :640].reshape(8, 32, 640)
    total[:, 1] = both[:, 640:].reshape(8, 32, 640)
    total[:, 2] = lax.dot_general(
        cols[1].reshape(1024, 256), hidden[...].reshape(1024, 640), dims, preferred_element_type=F32
    ).reshape(8, 32, 640)
    odd = z & 1
    near = jnp.where(odd == 1, z + 1, z - 1) & 7
    near = jnp.where(c == 0, z ^ 1, near)
    for k in range(4):
        keep[k] = total[((z >> 1) + k & 3) * 2 + odd]
        send[k] = total[((near >> 1) + k & 3) * 2 + (1 - odd)].astype(BF16)


def all_steps(tokens, grad_out, w_gate, w_lin, w_out_t, code, decode, stragglers):
    own = message(code, decode, stragglers, tokens, grad_out)
    row = [own] + [across(own, k, True) for k in (1, 2, 3)]
    w_in, w_out, token = loaded_weights(w_gate, w_lin, w_out_t)
    row, _ = lax.optimization_barrier((jnp.stack(row), token))
    near = [row]
    for k in (1, 2, 3):
        near.append(across(row, k, False))
    swap = sibling(row)
    *state, rows = gathered(0, (row, swap), w_in, w_out, ())
    state, near[1], near[3] = lax.optimization_barrier((state, near[1], near[3]))
    other = {k: sibling(near[k]) for k in (1, 3)}
    *state, rows = gathered(1, (near[1], other[1]), w_in, w_out, (*state, rows))
    planes = [rows] + [z_step(rows, j) for j in (1, 2, 3, 4)]
    state = gathered(3, (near[3], other[3]), w_in, w_out, state)
    state, near[2] = lax.optimization_barrier((state, near[2]))
    swap = sibling(near[2])
    state = gathered(2, (near[2],), w_in, w_out, state)
    keep, send = finished(2, swap, w_in, w_out, state, planes)
    got = z_pair(send)
    mixed = keep + got.astype(F32)
    result = mixed[0]
    for k in (2, 1, 3):
        result = result + z_step(mixed[k].astype(BF16), 2 * k).astype(F32)
    return jnp.transpose(result, (1, 0, 2))


def solution(mesh):
    split = Mesh(mesh.devices.reshape(2, 4, 8, 2, 2), ("xl", "y", "z", "xh", "c"))
    mp = ("xh", "c")
    in_specs = (P(BLK, mp), P(BLK, mp), P(None, mp), P(None, mp), P(None, mp), P(BLK, None), P(BLK), P())
    return jax.shard_map(all_steps, mesh=split, in_specs=in_specs, out_specs=P(BLK, None, mp), check_vma=False)
```

```python
import jax
import jax.numpy as jnp
from jax import lax
from jax.experimental import pallas as pl
from jax.experimental.pallas import tpu as pltpu
from jax.sharding import Mesh, PartitionSpec as P


BF16 = jnp.bfloat16
F32 = jnp.float32
I32 = jnp.int32
ROOT_2_PI = 0.7978845608028654
CUBIC = 0.044715
BLK = ("xl", "y", "z")
PLANE = ("xl", "y", "xh", "c")
SMEM = pl.BlockSpec(memory_space=pltpu.SMEM)
VMEM = pl.BlockSpec(memory_space=pltpu.VMEM)
PARAMS = pltpu.CompilerParams(vmem_limit_bytes=16 * 1024 * 1024)


def place():
    return [lax.axis_index(a).astype(I32) for a in ("xl", "y", "z", "xh", "c")]


def across(block, flip, first):
    route = []
    for xl in range(2):
        for y in range(4):
            for xh in range(2):
                for c in range(2):
                    on_x = (c == 0) == first
                    to = (xl ^ (flip & 1), y, xh ^ (flip >> 1), c) if on_x else (xl, y ^ flip, xh, c)
                    number = lambda a: ((a[0] * 4 + a[1]) * 2 + a[2]) * 2 + a[3]
                    route.append((number((xl, y, xh, c)), number(to)))
    return lax.ppermute(block, PLANE, route)


def swapped(block, axis, size, flip):
    return lax.ppermute(block, axis, [(i, i ^ flip) for i in range(size)])


def sibling(block):
    return lax.ppermute(block, "c", [(0, 1), (1, 0)])


def partner_of(z, c):
    return z ^ 1 if c == 0 else ((z + 1) % 8 if z % 2 else (z - 1) % 8)


def z_pair(block):
    return lax.ppermute(block, ("z", "c"), [(z * 2 + c, partner_of(z, c) * 2 + c) for z in range(8) for c in range(2)])


def z_step(block, step):
    return lax.ppermute(block, "z", [(z, (z + step) % 8) for z in range(8)])


def hbm(array):
    return pltpu.with_memory_space_constraint(array, pltpu.HBM)


def message_kernel(decode, code_in, stragglers_in, tokens, grad_out, out, code, stragglers, sems):
    pairs = (
        (tokens, out.at[pl.ds(0, 128)]),
        (grad_out, out.at[pl.ds(128, 128)]),
        (code_in, code),
        (stragglers_in, stragglers),
    )
    copies = [pltpu.make_async_copy(source, target, sems.at[i]) for i, (source, target) in enumerate(pairs)]
    for copy in copies:
        copy.start()
    for copy in copies[2:]:
        copy.wait()
    xl, y, z, _, _ = place()
    device = (xl * 4 + y) * 8 + z
    alive = stragglers[0] != device
    for i in range(1, 4):
        alive = alive & (stragglers[i] != device)
    scale = jnp.where(alive, decode[0], 0.0)
    lane = lax.broadcasted_iota(I32, (8, 128), 1)
    row = lax.broadcasted_iota(I32, (8, 128), 0)
    value = jnp.zeros((8, 128), F32)
    for j in range(5):
        value = jnp.where(lane == j, scale * code[0, j], value)
    high = value.astype(BF16).astype(F32)
    rest = value - high
    middle = rest.astype(BF16).astype(F32)
    low = rest - middle
    pieces = jnp.where(row == 0, high, jnp.where(row == 1, middle, jnp.where(row == 2, low, 0.0)))
    out[256:264, :] = jnp.zeros((8, 512), BF16)
    out[256:264, 0:128] = pieces.astype(BF16)
    for copy in copies[:2]:
        copy.wait()


def message(code, decode, stragglers, tokens, grad_out):
    return pl.pallas_call(
        message_kernel,
        out_shape=jax.ShapeDtypeStruct((264, 512), BF16),
        in_specs=[SMEM] + [pl.BlockSpec(memory_space=pltpu.HBM)] * 4,
        out_specs=VMEM,
        scratch_shapes=[pltpu.SMEM((1, 5), F32), pltpu.SMEM((4,), I32), pltpu.SemaphoreType.DMA((4,))],
        compiler_params=PARAMS,
        name="message",
    )(decode, *[hbm(a) for a in (code, stragglers, tokens, grad_out)])


def weights_kernel(w_gate, w_lin, w_out_t, w_in, w_out, sems):
    copies = [
        pltpu.make_async_copy(w_gate, w_in.at[:, :, pl.ds(0, 640)], sems.at[0]),
        pltpu.make_async_copy(w_lin, w_in.at[:, :, pl.ds(640, 640)], sems.at[1]),
        pltpu.make_async_copy(w_out_t, w_out, sems.at[2]),
    ]
    for copy in copies:
        copy.start()
    for copy in copies:
        copy.wait()


def loaded_weights(w_gate, w_lin, w_out_t):
    return pl.pallas_call(
        weights_kernel,
        out_shape=(
            jax.ShapeDtypeStruct((4, 512, 1280), BF16),
            jax.ShapeDtypeStruct((4, 512, 640), BF16),
        ),
        in_specs=[pl.BlockSpec(memory_space=pltpu.HBM)] * 3,
        out_specs=(VMEM, VMEM),
        scratch_shapes=[pltpu.SemaphoreType.DMA((3,))],
        compiler_params=PARAMS,
        name="load",
    )(*[hbm(w.reshape(4, 512, 640)) for w in (w_gate, w_lin, w_out_t)])


def rows_kernel(own, other, rows):
    c = lax.axis_index("c").astype(I32)
    rows[...] = jnp.zeros_like(rows)
    for dy in range(4):
        piece = [block[dy, 256:264, 0:128].astype(F32) for block in (own, other)]
        piece = jnp.where(c == 1, piece[0], piece[1])
        rows[dy : dy + 1, :] = jnp.sum(piece, axis=0, keepdims=True)


def line_rows(own, other):
    return pl.pallas_call(
        rows_kernel,
        out_shape=jax.ShapeDtypeStruct((8, 128), F32),
        in_specs=[VMEM] * 2,
        out_specs=VMEM,
        compiler_params=PARAMS,
        name="rows",
    )(own, other)


def first_kernel(own, other, w_in, w_out, acc, cols):
    acc[...] = jnp.zeros_like(acc)
    gather_kernel(0, ((0, own), (1, other)), w_in, w_out, acc, cols)


def middle_kernel(m, *refs):
    *blocks, w_in, w_out, _, __, acc, cols = refs
    gather_kernel(m, tuple(enumerate(blocks)), w_in, w_out, acc, cols)


def halves_kernel(low, high, w_in, w_out, _, __, acc, cols):
    gather_kernel(2, ((0, (low, high)),), w_in, w_out, acc, cols)


def final_kernel(low, high, w_in, w_out, _, __, own_terms, other_terms, acc, cols, *rest):
    gather_kernel(2, ((1, (low, high)),), w_in, w_out, acc, cols)
    last_kernel((own_terms, other_terms), acc, cols, *rest)


def gather_kernel(m, blocks, w_in, w_out, acc, cols):
    xl, y, _, xh, c = place()
    for ec, block in blocks:
        x_first = (c ^ ec) == 0

        def step(j, block, start):
            eh = jnp.where(x_first, j, m >> 1)
            p0 = jnp.where(x_first, 2 * m, 4 * j + (m & 1))
            p1 = jnp.where(x_first, 2 * m + 1, 4 * j + 2 + (m & 1))
            shard = (xh ^ eh) * 2 + (c ^ ec)
            xs = block[pl.ds(start, 2), 0:128].reshape(256, 512)
            ys = block[pl.ds(start, 2), 128:256].reshape(256, 512)
            pre = jnp.dot(xs, w_in[shard], preferred_element_type=F32)
            acc[0, p0] += pre[:128, :640]
            acc[1, p0] += pre[:128, 640:]
            acc[0, p1] += pre[128:, :640]
            acc[1, p1] += pre[128:, 640:]
            dh = jnp.dot(ys, w_out[shard], preferred_element_type=F32)
            acc[2, p0] += dh[:128]
            acc[2, p1] += dh[128:]

            @pl.when((ec == ((y >> 1) ^ c)) & (eh == (xl ^ xh)))
            def _():
                low = (y & 1) == 0
                for n, v in ((0, xs), (1, ys)):
                    v = jnp.where(low, v[:, :256], v[:, 256:])
                    cols[n, p0] = v[:128]
                    cols[n, p1] = v[128:]

        if isinstance(block, tuple):
            for j in range(2):
                step(j, block[j], 0)
        else:

            def body(j, carry):
                step(j, block, 2 * j)
                return carry

            lax.fori_loop(0, 2, body, 0)


STATE = (jax.ShapeDtypeStruct((3, 8, 128, 640), F32), jax.ShapeDtypeStruct((2, 8, 128, 256), BF16))


def priced(giga):
    return pl.CostEstimate(flops=giga << 30, bytes_accessed=1 << 20, transcendentals=0)


def gathered(m, blocks, w_in, w_out, state):
    n = len(blocks) + 2
    kernels = {0: first_kernel, 2: halves_kernel}
    return pl.pallas_call(
        kernels.get(m, lambda *refs: middle_kernel(m, *refs)),
        out_shape=STATE,
        in_specs=[VMEM] * (n + len(state)),
        out_specs=(VMEM, VMEM),
        input_output_aliases={n: 0, n + 1: 1} if state else {},
        compiler_params=PARAMS,
        cost_estimate=priced(2 if m != 2 else 1),
    )(*blocks, w_in, w_out, *state)


def finished(halves, w_in, w_out, state, terms):
    return pl.pallas_call(
        final_kernel,
        out_shape=STATE
        + (jax.ShapeDtypeStruct((4, 3, 32, 640), F32), jax.ShapeDtypeStruct((4, 3, 32, 640), BF16)),
        in_specs=[VMEM] * 8,
        out_specs=(VMEM,) * 4,
        input_output_aliases={4: 0, 5: 1},
        scratch_shapes=[
            pltpu.VMEM((8, 128, 1280), BF16),
            pltpu.VMEM((8, 128, 640), BF16),
            pltpu.VMEM((8, 3, 32, 640), F32),
        ],
        compiler_params=PARAMS,
        cost_estimate=priced(4),
        name="finish",
    )(*halves, w_in, w_out, *state, *terms)[2:]


def last_kernel(terms, acc, cols, keep, send, gates, hidden, total):
    xl, y, z, _, c = place()
    lane = lax.broadcasted_iota(I32, (8, 128), 1)
    row = lax.broadcasted_iota(I32, (8, 128), 0)
    known = (lane < 5) & (row < 4)
    workers = [(((xl ^ ex) * 4 + (y ^ row)) & 7) * 8 + ((z - lane) & 7) for ex in range(2)]

    def part(p, _):
        dy, ex = p >> 1, p & 1
        number = ((xl ^ ex) * 4 + (y ^ dy)) * 8 + z
        w = F32(0.0)
        for worker, term in zip(workers, terms):
            mine = known & (((number - lane) & 63) == worker)
            w = w + jnp.sum(jnp.where(mine, term[...], 0.0))
        for r in range(0, 128, 32):
            rows = pl.ds(r, 32)
            u = acc[0, p, rows]
            v = acc[1, p, rows]
            d = acc[2, p, rows] * w
            square = u * u
            t = jnp.tanh(ROOT_2_PI * (u + CUBIC * (square * u)))
            cdf = 0.5 * (1.0 + t)
            act = u * cdf
            slope = cdf + 0.5 * u * (1.0 - t * t) * (ROOT_2_PI * (1.0 + 3.0 * CUBIC * square))
            gates[p, rows, 0:640] = (d * v * slope).astype(BF16)
            gates[p, rows, 640:1280] = (d * act).astype(BF16)
            hidden[p, rows] = (act * v * w).astype(BF16)
        return 0

    lax.fori_loop(0, 8, part, 0)
    dims = (((0,), (0,)), ((), ()))
    both = lax.dot_general(
        cols[0].reshape(1024, 256), gates[...].reshape(1024, 1280), dims, preferred_element_type=F32
    )
    total[:, 0] = both[:, :640].reshape(8, 32, 640)
    total[:, 1] = both[:, 640:].reshape(8, 32, 640)
    total[:, 2] = lax.dot_general(
        cols[1].reshape(1024, 256), hidden[...].reshape(1024, 640), dims, preferred_element_type=F32
    ).reshape(8, 32, 640)
    odd = z & 1
    near = jnp.where(odd == 1, z + 1, z - 1) & 7
    near = jnp.where(c == 0, z ^ 1, near)
    for k in range(4):
        keep[k] = total[((z >> 1) + k & 3) * 2 + odd]
        send[k] = total[((near >> 1) + k & 3) * 2 + (1 - odd)].astype(BF16)


def all_steps(tokens, grad_out, w_gate, w_lin, w_out_t, code, decode, stragglers):
    own = message(code, decode, stragglers, tokens, grad_out)
    row = [own]
    for k in (1, 2, 3):
        row.append(across(own, k, True))
    w_in, w_out = loaded_weights(w_gate, w_lin, w_out_t)
    row = jnp.stack(row)
    near = {}
    for k in (1, 3):
        near[k] = across(row, k, False)
    swap = sibling(row)
    planes = [line_rows(row, swap)]
    for j in (1, 2, 3, 4):
        planes.append(z_step(planes[0], j))
    lane = lax.broadcasted_iota(I32, (8, 128), 1)
    terms = sum(jnp.where(lane == j, plane, 0.0) for j, plane in enumerate(planes))
    terms = (terms, swapped(terms, "xl", 2, 1))
    low = across(near[1][:2], 3, False)
    high = across(near[3][2:], 1, False)
    other = {}
    for k in (1, 3):
        other[k] = sibling(near[k])
    state = gathered(0, (row, swap), w_in, w_out, ())
    for m in (1, 3):
        state = gathered(m, (near[m], other[m]), w_in, w_out, state)
    state, low, high = lax.optimization_barrier((state, low, high))
    halves = [sibling(low), sibling(high)]
    state = gathered(2, (low, high), w_in, w_out, state)
    keep, send = finished(halves, w_in, w_out, state, terms)
    got = z_pair(send)
    mixed = keep + got.astype(F32)
    result = mixed[0]
    for k in (2, 1, 3):
        result = result + z_step(mixed[k].astype(BF16), 2 * k).astype(F32)
    return jnp.transpose(result, (1, 0, 2))


def solution(mesh):
    split = Mesh(mesh.devices.reshape(2, 4, 8, 2, 2), ("xl", "y", "z", "xh", "c"))
    mp = ("xh", "c")
    in_specs = (P(BLK, mp), P(BLK, mp), P(None, mp), P(None, mp), P(None, mp), P(BLK, None), P(BLK), P())
    return jax.shard_map(all_steps, mesh=split, in_specs=in_specs, out_specs=P(BLK, None, mp), check_vma=False)
```

```python
import jax
import jax.numpy as jnp
from jax import lax
from jax.experimental import pallas as pl
from jax.experimental.pallas import tpu as pltpu
from jax.sharding import Mesh, PartitionSpec as P


BF16 = jnp.bfloat16
F32 = jnp.float32
I32 = jnp.int32
ROOT_2_PI = 0.7978845608028654
CUBIC = 0.044715
BLK = ("xl", "y", "z")
PLANE = ("xl", "y", "xh", "c")
SMEM = pl.BlockSpec(memory_space=pltpu.SMEM)
VMEM = pl.BlockSpec(memory_space=pltpu.VMEM)
PARAMS = pltpu.CompilerParams(vmem_limit_bytes=16 * 1024 * 1024)


def place():
    return [lax.axis_index(a).astype(I32) for a in ("xl", "y", "z", "xh", "c")]


def across(block, flip, first):
    route = []
    for xl in range(2):
        for y in range(4):
            for xh in range(2):
                for c in range(2):
                    on_x = (c == 0) == first
                    to = (xl ^ (flip & 1), y, xh ^ (flip >> 1), c) if on_x else (xl, y ^ flip, xh, c)
                    number = lambda a: ((a[0] * 4 + a[1]) * 2 + a[2]) * 2 + a[3]
                    route.append((number((xl, y, xh, c)), number(to)))
    return lax.ppermute(block, PLANE, route)


def swapped(block, axis, size, flip):
    return lax.ppermute(block, axis, [(i, i ^ flip) for i in range(size)])


def sibling(block):
    return lax.ppermute(block, "c", [(0, 1), (1, 0)])


def partner_of(z, c):
    return z ^ 1 if c == 0 else ((z + 1) % 8 if z % 2 else (z - 1) % 8)


def z_pair(block):
    return lax.ppermute(block, ("z", "c"), [(z * 2 + c, partner_of(z, c) * 2 + c) for z in range(8) for c in range(2)])


def z_shift(block, step):
    return lax.ppermute(
        block, ("z", "c"), [(z * 2 + c, (z + step + c) % 8 * 2 + c) for z in range(8) for c in range(2)]
    )


def z_step(block, step):
    return lax.ppermute(block, "z", [(z, (z + step) % 8) for z in range(8)])


def hbm(array):
    return pltpu.with_memory_space_constraint(array, pltpu.HBM)


def message_kernel(decode, code_in, stragglers_in, tokens, grad_out, out, code, stragglers, sems):
    pairs = (
        (tokens, out.at[pl.ds(0, 128)]),
        (grad_out, out.at[pl.ds(128, 128)]),
        (code_in, code),
        (stragglers_in, stragglers),
    )
    copies = [pltpu.make_async_copy(source, target, sems.at[i]) for i, (source, target) in enumerate(pairs)]
    for copy in copies:
        copy.start()
    for copy in copies[2:]:
        copy.wait()
    xl, y, z, _, _ = place()
    device = (xl * 4 + y) * 8 + z
    alive = stragglers[0] != device
    for i in range(1, 4):
        alive = alive & (stragglers[i] != device)
    scale = jnp.where(alive, decode[0], 0.0)
    lane = lax.broadcasted_iota(I32, (8, 128), 1)
    row = lax.broadcasted_iota(I32, (8, 128), 0)
    value = jnp.zeros((8, 128), F32)
    for j in range(5):
        value = jnp.where(lane == j, scale * code[0, j], value)
    high = value.astype(BF16).astype(F32)
    rest = value - high
    middle = rest.astype(BF16).astype(F32)
    low = rest - middle
    pieces = jnp.where(row == 0, high, jnp.where(row == 1, middle, jnp.where(row == 2, low, 0.0)))
    out[256:264, :] = jnp.zeros((8, 512), BF16)
    out[256:264, 0:128] = pieces.astype(BF16)
    for copy in copies[:2]:
        copy.wait()


def message(code, decode, stragglers, tokens, grad_out):
    return pl.pallas_call(
        message_kernel,
        out_shape=jax.ShapeDtypeStruct((264, 512), BF16),
        in_specs=[SMEM] + [pl.BlockSpec(memory_space=pltpu.HBM)] * 4,
        out_specs=VMEM,
        scratch_shapes=[pltpu.SMEM((1, 5), F32), pltpu.SMEM((4,), I32), pltpu.SemaphoreType.DMA((4,))],
        compiler_params=PARAMS,
        name="message",
    )(decode, *[hbm(a) for a in (code, stragglers, tokens, grad_out)])


def weights_kernel(w_gate, w_lin, w_out_t, w_in, w_out, sems):
    copies = [
        pltpu.make_async_copy(w_gate, w_in.at[:, :, pl.ds(0, 640)], sems.at[0]),
        pltpu.make_async_copy(w_lin, w_in.at[:, :, pl.ds(640, 640)], sems.at[1]),
        pltpu.make_async_copy(w_out_t, w_out, sems.at[2]),
    ]
    for copy in copies:
        copy.start()
    for copy in copies:
        copy.wait()


def loaded_weights(w_gate, w_lin, w_out_t):
    return pl.pallas_call(
        weights_kernel,
        out_shape=(
            jax.ShapeDtypeStruct((4, 512, 1280), BF16),
            jax.ShapeDtypeStruct((4, 512, 640), BF16),
        ),
        in_specs=[pl.BlockSpec(memory_space=pltpu.HBM)] * 3,
        out_specs=(VMEM, VMEM),
        scratch_shapes=[pltpu.SemaphoreType.DMA((3,))],
        compiler_params=PARAMS,
        name="load",
    )(*[hbm(w.reshape(4, 512, 640)) for w in (w_gate, w_lin, w_out_t)])


def rows_kernel(own_low, own_high, other_low, other_high, rows):
    c = lax.axis_index("c").astype(I32)
    rows[...] = jnp.zeros_like(rows)
    for dy in range(4):
        pair = (own_low, other_low) if dy < 2 else (own_high, other_high)
        piece = [block[dy % 2, 256:264, 0:128].astype(F32) for block in pair]
        piece = jnp.where(c == 1, piece[0], piece[1])
        rows[dy : dy + 1, :] = jnp.sum(piece, axis=0, keepdims=True)


def line_rows(*blocks):
    return pl.pallas_call(
        rows_kernel,
        out_shape=jax.ShapeDtypeStruct((8, 128), F32),
        in_specs=[VMEM] * 4,
        out_specs=VMEM,
        compiler_params=PARAMS,
        name="rows",
    )(*blocks)


def add_block(m, j, ec, block, w_in, w_out, acc, cols):
    xl, y, _, xh, c = place()
    x_first = (c ^ ec) == 0
    eh = jnp.where(x_first, j, m >> 1)
    p0 = jnp.where(x_first, 2 * m, 4 * j + (m & 1))
    p1 = jnp.where(x_first, 2 * m + 1, 4 * j + 2 + (m & 1))
    shard = (xh ^ eh) * 2 + (c ^ ec)
    xs = block[:, 0:128].reshape(256, 512)
    ys = block[:, 128:256].reshape(256, 512)
    pre = jnp.dot(xs, w_in[shard], preferred_element_type=F32)
    acc[0, p0] += pre[:128, :640]
    acc[1, p0] += pre[:128, 640:]
    acc[0, p1] += pre[128:, :640]
    acc[1, p1] += pre[128:, 640:]
    dh = jnp.dot(ys, w_out[shard], preferred_element_type=F32)
    acc[2, p0] += dh[:128]
    acc[2, p1] += dh[128:]

    @pl.when((ec == ((y >> 1) ^ c)) & (eh == (xl ^ xh)))
    def _():
        low = (y & 1) == 0
        for n, v in ((0, xs), (1, ys)):
            v = jnp.where(low, v[:, :256], v[:, 256:])
            cols[n, p0] = v[:128]
            cols[n, p1] = v[128:]


STATE = (jax.ShapeDtypeStruct((3, 8, 128, 640), F32), jax.ShapeDtypeStruct((2, 8, 128, 256), BF16))


def priced(giga):
    return pl.CostEstimate(flops=giga << 30, bytes_accessed=1 << 20, transcendentals=0)


def gathered(items, w_in, w_out, state):
    n = len(items)

    def kernel(*refs):
        blocks, (w_in, w_out), (acc, cols) = refs[:n], refs[n : n + 2], refs[-2:]
        if not state:
            acc[...] = jnp.zeros_like(acc)
        for (m, j, ec, _), block in zip(items, blocks):
            add_block(m, j, ec, block, w_in, w_out, acc, cols)

    return pl.pallas_call(
        kernel,
        out_shape=STATE,
        in_specs=[VMEM] * (n + 2 + len(state)),
        out_specs=(VMEM, VMEM),
        input_output_aliases={n + 2: 0, n + 3: 1} if state else {},
        compiler_params=PARAMS,
        cost_estimate=priced(n // 2),
    )(*[item[3] for item in items], w_in, w_out, *state)


def finished(items, w_in, w_out, state, terms):
    n = len(items)

    def kernel(*refs):
        blocks, (w_in, w_out), terms = refs[:n], refs[n : n + 2], refs[n + 4 : n + 8]
        acc, cols, *rest = refs[n + 8 :]
        for (m, j, ec, _), block in zip(items, blocks):
            add_block(m, j, ec, block, w_in, w_out, acc, cols)
        last_kernel(terms, acc, cols, *rest)

    return pl.pallas_call(
        kernel,
        out_shape=STATE
        + (jax.ShapeDtypeStruct((4, 3, 32, 640), F32), jax.ShapeDtypeStruct((4, 3, 32, 640), BF16)),
        in_specs=[VMEM] * (n + 8),
        out_specs=(VMEM,) * 4,
        input_output_aliases={n + 2: 0, n + 3: 1},
        scratch_shapes=[
            pltpu.VMEM((8, 128, 1280), BF16),
            pltpu.VMEM((8, 128, 640), BF16),
            pltpu.VMEM((8, 3, 32, 640), F32),
        ],
        compiler_params=PARAMS,
        cost_estimate=priced(4),
        name="finish",
    )(*[item[3] for item in items], w_in, w_out, *state, *terms)[2:]


def last_kernel(terms, acc, cols, keep, send, gates, hidden, total):
    xl, y, z, _, c = place()
    lane = lax.broadcasted_iota(I32, (8, 128), 1)
    row = lax.broadcasted_iota(I32, (8, 128), 0)
    known = (lane < 5) & (row < 4)
    workers = [(((xl ^ ex) * 4 + (y ^ row)) & 7) * 8 + ((z - lane) & 7) for ex in range(2)]

    def part(p, _):
        dy, ex = p >> 1, p & 1
        number = ((xl ^ ex) * 4 + (y ^ dy)) * 8 + z
        w = F32(0.0)
        for i, worker in enumerate(workers):
            mine = known & (((number - lane) & 63) == worker)
            w = w + jnp.sum(jnp.where(mine, terms[2 * i][...] + terms[2 * i + 1][...], 0.0))
        for r in range(0, 128, 32):
            rows = pl.ds(r, 32)
            u = acc[0, p, rows]
            v = acc[1, p, rows]
            d = acc[2, p, rows] * w
            square = u * u
            t = jnp.tanh(ROOT_2_PI * (u + CUBIC * (square * u)))
            cdf = 0.5 * (1.0 + t)
            act = u * cdf
            slope = cdf + 0.5 * u * (1.0 - t * t) * (ROOT_2_PI * (1.0 + 3.0 * CUBIC * square))
            gates[p, rows, 0:640] = (d * v * slope).astype(BF16)
            gates[p, rows, 640:1280] = (d * act).astype(BF16)
            hidden[p, rows] = (act * v * w).astype(BF16)
        return 0

    lax.fori_loop(0, 8, part, 0)
    dims = (((0,), (0,)), ((), ()))
    both = lax.dot_general(
        cols[0].reshape(1024, 256), gates[...].reshape(1024, 1280), dims, preferred_element_type=F32
    )
    total[:, 0] = both[:, :640].reshape(8, 32, 640)
    total[:, 1] = both[:, 640:].reshape(8, 32, 640)
    total[:, 2] = lax.dot_general(
        cols[1].reshape(1024, 256), hidden[...].reshape(1024, 640), dims, preferred_element_type=F32
    ).reshape(8, 32, 640)
    odd = z & 1
    near = jnp.where(odd == 1, z + 1, z - 1) & 7
    near = jnp.where(c == 0, z ^ 1, near)
    for k in range(4):
        keep[k] = total[((z >> 1) + k & 3) * 2 + odd]
        send[k] = total[((near >> 1) + k & 3) * 2 + (1 - odd)].astype(BF16)


def all_steps(tokens, grad_out, w_gate, w_lin, w_out_t, code, decode, stragglers):
    own = message(code, decode, stragglers, tokens, grad_out)
    first = {}
    for k in (1, 2, 3):
        first[k] = across(own, k, True)
    w_in, w_out = loaded_weights(w_gate, w_lin, w_out_t)
    low, high = jnp.stack([own, first[1]]), jnp.stack([first[2], first[3]])
    blocks, others = {(0, 0): low, (0, 1): high}, {}
    for j, half in enumerate((low, high)):
        for k in (1, 3):
            blocks[k, j] = across(half, k, False)
        others[0, j] = sibling(half)
    for j, came, flip in ((0, 1, 3), (1, 3, 1)):
        blocks[2, j] = across(blocks[came, j], flip, False)
    rows = line_rows(low, high, others[0, 0], others[0, 1])
    c = lax.axis_index("c").astype(I32)
    lane = lax.broadcasted_iota(I32, (8, 128), 1)
    partial = jnp.where((lane == 0) & (c == 0), rows, 0.0)
    for j in (1, 3):
        partial = partial + jnp.where(lane == j + c, z_shift(rows, j), 0.0)
    partials = [partial, swapped(partial, "xl", 2, 1)]
    terms = []
    for part in partials:
        terms += [part, sibling(part)]
    for j in range(2):
        for k in (1, 3):
            others[k, j] = sibling(blocks[k, j])

    def items(keys, sides=(0, 1)):
        return [(m, j, ec, (blocks, others)[ec][m, j]) for m, j in keys for ec in sides]

    state = gathered(items([(0, 0), (0, 1)]), w_in, w_out, ())
    for j in range(2):
        state = gathered(items([(1, j), (3, j)]), w_in, w_out, state)
    state, blocks[2, 0], blocks[2, 1] = lax.optimization_barrier((state, blocks[2, 0], blocks[2, 1]))
    for j in range(2):
        others[2, j] = sibling(blocks[2, j])
    far = [(2, 0), (2, 1)]
    state = gathered(items(far, (0,)), w_in, w_out, state)
    keep, send = finished(items(far, (1,)), w_in, w_out, state, terms)
    got = z_pair(send)
    mixed = keep + got.astype(F32)
    result = mixed[0]
    for k in (2, 1, 3):
        result = result + z_step(mixed[k].astype(BF16), 2 * k).astype(F32)
    return jnp.transpose(result, (1, 0, 2))


def solution(mesh):
    split = Mesh(mesh.devices.reshape(2, 4, 8, 2, 2), ("xl", "y", "z", "xh", "c"))
    mp = ("xh", "c")
    in_specs = (P(BLK, mp), P(BLK, mp), P(None, mp), P(None, mp), P(None, mp), P(BLK, None), P(BLK), P())
    return jax.shard_map(all_steps, mesh=split, in_specs=in_specs, out_specs=P(BLK, None, mp), check_vma=False)
```

```python
import jax
import jax.numpy as jnp
from jax import lax
from jax.experimental import pallas as pl
from jax.experimental.pallas import tpu as pltpu
from jax.sharding import Mesh, PartitionSpec as P


BF16 = jnp.bfloat16
F32 = jnp.float32
I32 = jnp.int32
ROOT_2_PI = 0.7978845608028654
CUBIC = 0.044715
BLK = ("xl", "y", "z")
PLANE = ("xl", "y", "xh", "c")
SMEM = pl.BlockSpec(memory_space=pltpu.SMEM)
VMEM = pl.BlockSpec(memory_space=pltpu.VMEM)
PARAMS = pltpu.CompilerParams(vmem_limit_bytes=16 * 1024 * 1024)


def place():
    return [lax.axis_index(a).astype(I32) for a in ("xl", "y", "z", "xh", "c")]


def across(block, flip, first):
    route = []
    for xl in range(2):
        for y in range(4):
            for xh in range(2):
                for c in range(2):
                    on_x = (c == 0) == first
                    to = (xl ^ (flip & 1), y, xh ^ (flip >> 1), c) if on_x else (xl, y ^ flip, xh, c)
                    number = lambda a: ((a[0] * 4 + a[1]) * 2 + a[2]) * 2 + a[3]
                    route.append((number((xl, y, xh, c)), number(to)))
    return lax.ppermute(block, PLANE, route)


def swapped(block, axis, size, flip):
    return lax.ppermute(block, axis, [(i, i ^ flip) for i in range(size)])


def sibling(block):
    return lax.ppermute(block, "c", [(0, 1), (1, 0)])


def partner_of(z, c):
    return z ^ 1 if c == 0 else ((z + 1) % 8 if z % 2 else (z - 1) % 8)


def z_pair(block):
    return lax.ppermute(block, ("z", "c"), [(z * 2 + c, partner_of(z, c) * 2 + c) for z in range(8) for c in range(2)])


def z_shift(block, step):
    return lax.ppermute(
        block, ("z", "c"), [(z * 2 + c, (z + step + c) % 8 * 2 + c) for z in range(8) for c in range(2)]
    )


def z_step(block, step):
    return lax.ppermute(block, "z", [(z, (z + step) % 8) for z in range(8)])


def hbm(array):
    return pltpu.with_memory_space_constraint(array, pltpu.HBM)


def message_kernel(decode, code_in, stragglers_in, tokens, grad_out, out, code, stragglers, sems):
    pairs = (
        (tokens, out.at[pl.ds(0, 128)]),
        (grad_out, out.at[pl.ds(128, 128)]),
        (code_in, code),
        (stragglers_in, stragglers),
    )
    copies = [pltpu.make_async_copy(source, target, sems.at[i]) for i, (source, target) in enumerate(pairs)]
    for copy in copies:
        copy.start()
    for copy in copies[2:]:
        copy.wait()
    xl, y, z, _, _ = place()
    device = (xl * 4 + y) * 8 + z
    alive = stragglers[0] != device
    for i in range(1, 4):
        alive = alive & (stragglers[i] != device)
    scale = jnp.where(alive, decode[0], 0.0)
    lane = lax.broadcasted_iota(I32, (8, 128), 1)
    row = lax.broadcasted_iota(I32, (8, 128), 0)
    value = jnp.zeros((8, 128), F32)
    for j in range(5):
        value = jnp.where(lane == j, scale * code[0, j], value)
    high = value.astype(BF16).astype(F32)
    rest = value - high
    middle = rest.astype(BF16).astype(F32)
    low = rest - middle
    pieces = jnp.where(row == 0, high, jnp.where(row == 1, middle, jnp.where(row == 2, low, 0.0)))
    out[256:264, :] = jnp.zeros((8, 512), BF16)
    out[256:264, 0:128] = pieces.astype(BF16)
    for copy in copies[:2]:
        copy.wait()


def message(code, decode, stragglers, tokens, grad_out):
    return pl.pallas_call(
        message_kernel,
        out_shape=jax.ShapeDtypeStruct((264, 512), BF16),
        in_specs=[SMEM] + [pl.BlockSpec(memory_space=pltpu.HBM)] * 4,
        out_specs=VMEM,
        scratch_shapes=[pltpu.SMEM((1, 5), F32), pltpu.SMEM((4,), I32), pltpu.SemaphoreType.DMA((4,))],
        compiler_params=PARAMS,
        name="message",
    )(decode, *[hbm(a) for a in (code, stragglers, tokens, grad_out)])


def weights_kernel(w_gate, w_lin, w_out_t, w_in, w_out, sems):
    copies = [
        pltpu.make_async_copy(w_gate, w_in.at[:, :, pl.ds(0, 640)], sems.at[0]),
        pltpu.make_async_copy(w_lin, w_in.at[:, :, pl.ds(640, 640)], sems.at[1]),
        pltpu.make_async_copy(w_out_t, w_out, sems.at[2]),
    ]
    for copy in copies:
        copy.start()
    for copy in copies:
        copy.wait()


def loaded_weights(w_gate, w_lin, w_out_t):
    return pl.pallas_call(
        weights_kernel,
        out_shape=(
            jax.ShapeDtypeStruct((4, 512, 1280), BF16),
            jax.ShapeDtypeStruct((4, 512, 640), BF16),
        ),
        in_specs=[pl.BlockSpec(memory_space=pltpu.HBM)] * 3,
        out_specs=(VMEM, VMEM),
        scratch_shapes=[pltpu.SemaphoreType.DMA((3,))],
        compiler_params=PARAMS,
        name="load",
    )(*[hbm(w.reshape(4, 512, 640)) for w in (w_gate, w_lin, w_out_t)])


def rows_kernel(own, other, rows):
    c = lax.axis_index("c").astype(I32)
    rows[...] = jnp.zeros_like(rows)
    for dy in range(4):
        piece = [block[dy, 256:264, 0:128].astype(F32) for block in (own, other)]
        piece = jnp.where(c == 1, piece[0], piece[1])
        rows[dy : dy + 1, :] = jnp.sum(piece, axis=0, keepdims=True)


def line_rows(own, other):
    return pl.pallas_call(
        rows_kernel,
        out_shape=jax.ShapeDtypeStruct((8, 128), F32),
        in_specs=[VMEM] * 2,
        out_specs=VMEM,
        compiler_params=PARAMS,
        name="rows",
    )(own, other)


def part_kernel(rows, near, far, out):
    c = lax.axis_index("c").astype(I32)
    lane = lax.broadcasted_iota(I32, (8, 128), 1)
    total = jnp.where((lane == 0) & (c == 0), rows[...], 0.0)
    total = jnp.where(lane == 1 + c, near[...], total)
    out[...] = jnp.where(lane == 3 + c, far[...], total)


def part_of_line(*rows):
    return pl.pallas_call(
        part_kernel,
        out_shape=jax.ShapeDtypeStruct((8, 128), F32),
        in_specs=[VMEM] * 3,
        out_specs=VMEM,
        compiler_params=PARAMS,
        name="part",
    )(*rows)


def first_kernel(own, other, w_in, w_out, acc, cols):
    acc[...] = jnp.zeros_like(acc)
    gather_kernel(0, ((0, own), (1, other)), w_in, w_out, acc, cols)


def middle_kernel(m, *refs):
    *blocks, w_in, w_out, _, __, acc, cols = refs
    gather_kernel(m, tuple(enumerate(blocks)), w_in, w_out, acc, cols)


def halves_kernel(low, high, w_in, w_out, _, __, acc, cols):
    gather_kernel(2, ((0, (low, high)),), w_in, w_out, acc, cols)


def final_kernel(low, high, w_in, w_out, _, __, *refs):
    terms, (acc, cols, *rest) = refs[:4], refs[4:]
    gather_kernel(2, ((1, (low, high)),), w_in, w_out, acc, cols)
    last_kernel(terms, acc, cols, *rest)


def gather_kernel(m, blocks, w_in, w_out, acc, cols):
    xl, y, _, xh, c = place()
    for ec, block in blocks:
        x_first = (c ^ ec) == 0

        def step(j, block, start):
            eh = jnp.where(x_first, j, m >> 1)
            p0 = jnp.where(x_first, 2 * m, 4 * j + (m & 1))
            p1 = jnp.where(x_first, 2 * m + 1, 4 * j + 2 + (m & 1))
            shard = (xh ^ eh) * 2 + (c ^ ec)
            xs = block[pl.ds(start, 2), 0:128].reshape(256, 512)
            ys = block[pl.ds(start, 2), 128:256].reshape(256, 512)
            pre = jnp.dot(xs, w_in[shard], preferred_element_type=F32)
            acc[0, p0] += pre[:128, :640]
            acc[1, p0] += pre[:128, 640:]
            acc[0, p1] += pre[128:, :640]
            acc[1, p1] += pre[128:, 640:]
            dh = jnp.dot(ys, w_out[shard], preferred_element_type=F32)
            acc[2, p0] += dh[:128]
            acc[2, p1] += dh[128:]

            @pl.when((ec == ((y >> 1) ^ c)) & (eh == (xl ^ xh)))
            def _():
                low = (y & 1) == 0
                for n, v in ((0, xs), (1, ys)):
                    v = jnp.where(low, v[:, :256], v[:, 256:])
                    cols[n, p0] = v[:128]
                    cols[n, p1] = v[128:]

        if isinstance(block, tuple):
            for j in range(2):
                step(j, block[j], 0)
        else:

            def body(j, carry):
                step(j, block, 2 * j)
                return carry

            lax.fori_loop(0, 2, body, 0)


STATE = (jax.ShapeDtypeStruct((3, 8, 128, 640), F32), jax.ShapeDtypeStruct((2, 8, 128, 256), BF16))


def priced(giga):
    return pl.CostEstimate(flops=giga << 30, bytes_accessed=1 << 20, transcendentals=0)


def gathered(m, blocks, w_in, w_out, state):
    n = len(blocks) + 2
    kernels = {0: first_kernel, 2: halves_kernel}
    return pl.pallas_call(
        kernels.get(m, lambda *refs: middle_kernel(m, *refs)),
        out_shape=STATE,
        in_specs=[VMEM] * (n + len(state)),
        out_specs=(VMEM, VMEM),
        input_output_aliases={n: 0, n + 1: 1} if state else {},
        compiler_params=PARAMS,
        cost_estimate=priced(2 if m != 2 else 1),
    )(*blocks, w_in, w_out, *state)


def finished(halves, w_in, w_out, state, terms):
    return pl.pallas_call(
        final_kernel,
        out_shape=STATE
        + (jax.ShapeDtypeStruct((4, 3, 32, 640), F32), jax.ShapeDtypeStruct((4, 3, 32, 640), BF16)),
        in_specs=[VMEM] * 10,
        out_specs=(VMEM,) * 4,
        input_output_aliases={4: 0, 5: 1},
        scratch_shapes=[
            pltpu.VMEM((8, 128, 1280), BF16),
            pltpu.VMEM((8, 128, 640), BF16),
            pltpu.VMEM((8, 3, 32, 640), F32),
        ],
        compiler_params=PARAMS,
        cost_estimate=priced(4),
        name="finish",
    )(*halves, w_in, w_out, *state, *terms)[2:]


def last_kernel(terms, acc, cols, keep, send, gates, hidden, total):
    xl, y, z, _, c = place()
    lane = lax.broadcasted_iota(I32, (8, 128), 1)
    row = lax.broadcasted_iota(I32, (8, 128), 0)
    known = (lane < 5) & (row < 4)
    workers = [(((xl ^ ex) * 4 + (y ^ row)) & 7) * 8 + ((z - lane) & 7) for ex in range(2)]

    def part(p, _):
        dy, ex = p >> 1, p & 1
        number = ((xl ^ ex) * 4 + (y ^ dy)) * 8 + z
        w = F32(0.0)
        for i, worker in enumerate(workers):
            mine = known & (((number - lane) & 63) == worker)
            w = w + jnp.sum(jnp.where(mine, terms[2 * i][...] + terms[2 * i + 1][...], 0.0))
        for r in range(0, 128, 32):
            rows = pl.ds(r, 32)
            u = acc[0, p, rows]
            v = acc[1, p, rows]
            d = acc[2, p, rows] * w
            square = u * u
            t = jnp.tanh(ROOT_2_PI * (u + CUBIC * (square * u)))
            cdf = 0.5 * (1.0 + t)
            act = u * cdf
            slope = cdf + 0.5 * u * (1.0 - t * t) * (ROOT_2_PI * (1.0 + 3.0 * CUBIC * square))
            gates[p, rows, 0:640] = (d * v * slope).astype(BF16)
            gates[p, rows, 640:1280] = (d * act).astype(BF16)
            hidden[p, rows] = (act * v * w).astype(BF16)
        return 0

    lax.fori_loop(0, 8, part, 0)
    dims = (((0,), (0,)), ((), ()))
    both = lax.dot_general(
        cols[0].reshape(1024, 256), gates[...].reshape(1024, 1280), dims, preferred_element_type=F32
    )
    total[:, 0] = both[:, :640].reshape(8, 32, 640)
    total[:, 1] = both[:, 640:].reshape(8, 32, 640)
    total[:, 2] = lax.dot_general(
        cols[1].reshape(1024, 256), hidden[...].reshape(1024, 640), dims, preferred_element_type=F32
    ).reshape(8, 32, 640)
    odd = z & 1
    near = jnp.where(odd == 1, z + 1, z - 1) & 7
    near = jnp.where(c == 0, z ^ 1, near)
    for k in range(4):
        keep[k] = total[((z >> 1) + k & 3) * 2 + odd]
        send[k] = total[((near >> 1) + k & 3) * 2 + (1 - odd)].astype(BF16)


def all_steps(tokens, grad_out, w_gate, w_lin, w_out_t, code, decode, stragglers):
    own = message(code, decode, stragglers, tokens, grad_out)
    row = [own]
    for k in (1, 2, 3):
        row.append(across(own, k, True))
    w_in, w_out = loaded_weights(w_gate, w_lin, w_out_t)
    row = jnp.stack(row)
    near = {}
    for k in (1, 3):
        near[k] = across(row, k, False)
    swap = sibling(row)
    rows = line_rows(row, swap)
    got = []
    for j in (1, 3):
        got.append(z_shift(rows, j))
    partial = part_of_line(rows, *got)
    partials = [partial, swapped(partial, "xl", 2, 1)]
    terms = []
    for part in partials:
        terms += [part, sibling(part)]
    low = across(near[1][:2], 3, False)
    high = across(near[3][2:], 1, False)
    other = {}
    for k in (1, 3):
        other[k] = sibling(near[k])
    state = gathered(0, (row, swap), w_in, w_out, ())
    for m in (1, 3):
        state = gathered(m, (near[m], other[m]), w_in, w_out, state)
    state, low, high = lax.optimization_barrier((state, low, high))
    halves = [sibling(low), sibling(high)]
    state = gathered(2, (low, high), w_in, w_out, state)
    keep, send = finished(halves, w_in, w_out, state, terms)
    got = z_pair(send)
    mixed = keep + got.astype(F32)
    result = mixed[0]
    for k in (2, 1, 3):
        result = result + z_step(mixed[k].astype(BF16), 2 * k).astype(F32)
    return jnp.transpose(result, (1, 0, 2))


def solution(mesh):
    split = Mesh(mesh.devices.reshape(2, 4, 8, 2, 2), ("xl", "y", "z", "xh", "c"))
    mp = ("xh", "c")
    in_specs = (P(BLK, mp), P(BLK, mp), P(None, mp), P(None, mp), P(None, mp), P(BLK, None), P(BLK), P())
    return jax.shard_map(all_steps, mesh=split, in_specs=in_specs, out_specs=P(BLK, None, mp), check_vma=False)
```

```python
import jax
import jax.numpy as jnp
from jax import lax
from jax.experimental import pallas as pl
from jax.experimental.pallas import tpu as pltpu
from jax.sharding import Mesh, PartitionSpec as P


BF16 = jnp.bfloat16
F32 = jnp.float32
I32 = jnp.int32
ROOT_2_PI = 0.7978845608028654
CUBIC = 0.044715
CUTS = ((0, 384), (384, 640))
BLK = ("xl", "y", "z")
PLANE = ("xl", "y", "xh", "c")
SMEM = pl.BlockSpec(memory_space=pltpu.SMEM)
VMEM = pl.BlockSpec(memory_space=pltpu.VMEM)
PARAMS = pltpu.CompilerParams(vmem_limit_bytes=16 * 1024 * 1024)


def place():
    return [lax.axis_index(a).astype(I32) for a in ("xl", "y", "z", "xh", "c")]


def across(block, flip, first):
    route = []
    for xl in range(2):
        for y in range(4):
            for xh in range(2):
                for c in range(2):
                    on_x = (c == 0) == first
                    to = (xl ^ (flip & 1), y, xh ^ (flip >> 1), c) if on_x else (xl, y ^ flip, xh, c)
                    number = lambda a: ((a[0] * 4 + a[1]) * 2 + a[2]) * 2 + a[3]
                    route.append((number((xl, y, xh, c)), number(to)))
    return lax.ppermute(block, PLANE, route)


def swapped(block, axis, size, flip):
    return lax.ppermute(block, axis, [(i, i ^ flip) for i in range(size)])


def sibling(block):
    return lax.ppermute(block, "c", [(0, 1), (1, 0)])


def partner_of(z, c):
    return z ^ 1 if c == 0 else ((z + 1) % 8 if z % 2 else (z - 1) % 8)


def z_pair(block):
    return lax.ppermute(block, ("z", "c"), [(z * 2 + c, partner_of(z, c) * 2 + c) for z in range(8) for c in range(2)])


def z_shift(block, step):
    return lax.ppermute(
        block, ("z", "c"), [(z * 2 + c, (z + step + c) % 8 * 2 + c) for z in range(8) for c in range(2)]
    )


def z_step(block, step):
    return lax.ppermute(block, "z", [(z, (z + step) % 8) for z in range(8)])


def hbm(array):
    return pltpu.with_memory_space_constraint(array, pltpu.HBM)


def message_kernel(decode, code_in, stragglers_in, tokens, grad_out, out, code, stragglers, sems):
    pairs = (
        (tokens, out.at[pl.ds(0, 128)]),
        (grad_out, out.at[pl.ds(128, 128)]),
        (code_in, code),
        (stragglers_in, stragglers),
    )
    copies = [pltpu.make_async_copy(source, target, sems.at[i]) for i, (source, target) in enumerate(pairs)]
    for copy in copies:
        copy.start()
    for copy in copies[2:]:
        copy.wait()
    xl, y, z, _, _ = place()
    device = (xl * 4 + y) * 8 + z
    alive = stragglers[0] != device
    for i in range(1, 4):
        alive = alive & (stragglers[i] != device)
    scale = jnp.where(alive, decode[0], 0.0)
    lane = lax.broadcasted_iota(I32, (8, 128), 1)
    row = lax.broadcasted_iota(I32, (8, 128), 0)
    value = jnp.zeros((8, 128), F32)
    for j in range(5):
        value = jnp.where(lane == j, scale * code[0, j], value)
    high = value.astype(BF16).astype(F32)
    rest = value - high
    middle = rest.astype(BF16).astype(F32)
    low = rest - middle
    pieces = jnp.where(row == 0, high, jnp.where(row == 1, middle, jnp.where(row == 2, low, 0.0)))
    out[256:264, :] = jnp.zeros((8, 512), BF16)
    out[256:264, 0:128] = pieces.astype(BF16)
    for copy in copies[:2]:
        copy.wait()


def message(code, decode, stragglers, tokens, grad_out):
    return pl.pallas_call(
        message_kernel,
        out_shape=jax.ShapeDtypeStruct((264, 512), BF16),
        in_specs=[SMEM] + [pl.BlockSpec(memory_space=pltpu.HBM)] * 4,
        out_specs=VMEM,
        scratch_shapes=[pltpu.SMEM((1, 5), F32), pltpu.SMEM((4,), I32), pltpu.SemaphoreType.DMA((4,))],
        compiler_params=PARAMS,
        name="message",
    )(decode, *[hbm(a) for a in (code, stragglers, tokens, grad_out)])


def weights_kernel(w_gate, w_lin, w_out_t, w_in, w_out, sems):
    pairs = [(w_out_t, w_out)]
    for lower, upper in CUTS:
        width = upper - lower
        for n, w in enumerate((w_gate, w_lin)):
            target = w_in.at[:, :, pl.ds(2 * lower + n * width, width)]
            pairs.append((w.at[:, :, pl.ds(lower, width)], target))
    copies = [pltpu.make_async_copy(*pair, sems.at[i]) for i, pair in enumerate(pairs)]
    for copy in copies:
        copy.start()
    for copy in copies:
        copy.wait()


def loaded_weights(w_gate, w_lin, w_out_t):
    return pl.pallas_call(
        weights_kernel,
        out_shape=(
            jax.ShapeDtypeStruct((4, 512, 1280), BF16),
            jax.ShapeDtypeStruct((4, 512, 640), BF16),
        ),
        in_specs=[pl.BlockSpec(memory_space=pltpu.HBM)] * 3,
        out_specs=(VMEM, VMEM),
        scratch_shapes=[pltpu.SemaphoreType.DMA((5,))],
        compiler_params=PARAMS,
        name="load",
    )(*[hbm(w.reshape(4, 512, 640)) for w in (w_gate, w_lin, w_out_t)])


def rows_kernel(own, other, rows):
    c = lax.axis_index("c").astype(I32)
    rows[...] = jnp.zeros_like(rows)
    for dy in range(4):
        piece = [block[dy, 256:264, 0:128].astype(F32) for block in (own, other)]
        piece = jnp.where(c == 1, piece[0], piece[1])
        rows[dy : dy + 1, :] = jnp.sum(piece, axis=0, keepdims=True)


def line_rows(own, other):
    return pl.pallas_call(
        rows_kernel,
        out_shape=jax.ShapeDtypeStruct((8, 128), F32),
        in_specs=[VMEM] * 2,
        out_specs=VMEM,
        compiler_params=PARAMS,
        name="rows",
    )(own, other)


def part_kernel(rows, near, far, out):
    c = lax.axis_index("c").astype(I32)
    lane = lax.broadcasted_iota(I32, (8, 128), 1)
    total = jnp.where((lane == 0) & (c == 0), rows[...], 0.0)
    total = jnp.where(lane == 1 + c, near[...], total)
    out[...] = jnp.where(lane == 3 + c, far[...], total)


def part_of_line(*rows):
    return pl.pallas_call(
        part_kernel,
        out_shape=jax.ShapeDtypeStruct((8, 128), F32),
        in_specs=[VMEM] * 3,
        out_specs=VMEM,
        compiler_params=PARAMS,
        name="part",
    )(*rows)


def first_kernel(own, other, w_in, w_out, acc, cols):
    acc[...] = jnp.zeros_like(acc)
    gather_kernel(0, ((0, own), (1, other)), w_in, w_out, acc, cols)


def middle_kernel(m, *refs):
    *blocks, w_in, w_out, _, __, acc, cols = refs
    gather_kernel(m, tuple(enumerate(blocks)), w_in, w_out, acc, cols)


def halves_kernel(low, high, w_in, w_out, _, __, acc, cols):
    gather_kernel(2, ((0, (low, high)),), w_in, w_out, acc, cols)


def final_kernel(cut, low, high, w_in, w_out, _, __, *refs):
    terms, (acc, cols, *rest) = refs[:4], refs[4:]
    gather_kernel(2, ((1, (low, high)),), w_in, w_out, acc, cols, (CUTS[cut],), cut == 0)
    last_kernel(CUTS[cut], terms, acc, cols, *rest)


def gather_kernel(m, blocks, w_in, w_out, acc, cols, cuts=CUTS, with_cols=True):
    xl, y, _, xh, c = place()
    for ec, block in blocks:
        x_first = (c ^ ec) == 0

        def step(j, block, start):
            eh = jnp.where(x_first, j, m >> 1)
            p0 = jnp.where(x_first, 2 * m, 4 * j + (m & 1))
            p1 = jnp.where(x_first, 2 * m + 1, 4 * j + 2 + (m & 1))
            shard = (xh ^ eh) * 2 + (c ^ ec)
            xs = block[pl.ds(start, 2), 0:128].reshape(256, 512)
            ys = block[pl.ds(start, 2), 128:256].reshape(256, 512)
            first, end = cuts[0][0], cuts[-1][1]
            pre = jnp.dot(xs, w_in[shard, :, 2 * first : 2 * end], preferred_element_type=F32)
            for lower, upper in cuts:
                width = upper - lower
                for n in range(2):
                    at = 2 * (lower - first) + n * width
                    acc[n, p0, :, lower:upper] += pre[:128, at : at + width]
                    acc[n, p1, :, lower:upper] += pre[128:, at : at + width]
            dh = jnp.dot(ys, w_out[shard, :, first:end], preferred_element_type=F32)
            acc[2, p0, :, first:end] += dh[:128]
            acc[2, p1, :, first:end] += dh[128:]
            if not with_cols:
                return

            @pl.when((ec == ((y >> 1) ^ c)) & (eh == (xl ^ xh)))
            def _():
                low = (y & 1) == 0
                for n, v in ((0, xs), (1, ys)):
                    v = jnp.where(low, v[:, :256], v[:, 256:])
                    cols[n, p0] = v[:128]
                    cols[n, p1] = v[128:]

        if isinstance(block, tuple):
            for j in range(2):
                step(j, block[j], 0)
        else:

            def body(j, carry):
                step(j, block, 2 * j)
                return carry

            lax.fori_loop(0, 2, body, 0)


STATE = (jax.ShapeDtypeStruct((3, 8, 128, 640), F32), jax.ShapeDtypeStruct((2, 8, 128, 256), BF16))


def priced(giga):
    return pl.CostEstimate(flops=giga << 30, bytes_accessed=1 << 20, transcendentals=0)


def gathered(m, blocks, w_in, w_out, state):
    n = len(blocks) + 2
    kernels = {0: first_kernel, 2: halves_kernel}
    return pl.pallas_call(
        kernels.get(m, lambda *refs: middle_kernel(m, *refs)),
        out_shape=STATE,
        in_specs=[VMEM] * (n + len(state)),
        out_specs=(VMEM, VMEM),
        input_output_aliases={n: 0, n + 1: 1} if state else {},
        compiler_params=PARAMS,
        cost_estimate=priced(2 if m != 2 else 1),
    )(*blocks, w_in, w_out, *state)


def finished(cut, halves, w_in, w_out, state, terms):
    width = CUTS[cut][1] - CUTS[cut][0]
    *state, keep, send = pl.pallas_call(
        lambda *refs: final_kernel(cut, *refs),
        out_shape=STATE
        + (jax.ShapeDtypeStruct((4, 3, 32, width), F32), jax.ShapeDtypeStruct((4, 3, 32, width), BF16)),
        in_specs=[VMEM] * 10,
        out_specs=(VMEM,) * 4,
        input_output_aliases={4: 0, 5: 1},
        scratch_shapes=[
            pltpu.VMEM((8, 128, 2 * width), BF16),
            pltpu.VMEM((8, 128, width), BF16),
            pltpu.VMEM((8, 3, 32, width), F32),
        ],
        compiler_params=PARAMS,
        cost_estimate=priced(2),
    )(*halves, w_in, w_out, *state, *terms)
    return state, keep, send


def last_kernel(cut, terms, acc, cols, keep, send, gates, hidden, total):
    xl, y, z, _, c = place()
    lane = lax.broadcasted_iota(I32, (8, 128), 1)
    lower, upper = cut
    width = upper - lower
    row = lax.broadcasted_iota(I32, (8, 128), 0)
    known = (lane < 5) & (row < 4)
    workers = [(((xl ^ ex) * 4 + (y ^ row)) & 7) * 8 + ((z - lane) & 7) for ex in range(2)]

    def part(p, _):
        dy, ex = p >> 1, p & 1
        number = ((xl ^ ex) * 4 + (y ^ dy)) * 8 + z
        w = F32(0.0)
        for i, worker in enumerate(workers):
            mine = known & (((number - lane) & 63) == worker)
            w = w + jnp.sum(jnp.where(mine, terms[2 * i][...] + terms[2 * i + 1][...], 0.0))
        for r in range(0, 128, 32):
            rows = pl.ds(r, 32)
            u = acc[0, p, rows, lower:upper]
            v = acc[1, p, rows, lower:upper]
            d = acc[2, p, rows, lower:upper] * w
            square = u * u
            t = jnp.tanh(ROOT_2_PI * (u + CUBIC * (square * u)))
            cdf = 0.5 * (1.0 + t)
            act = u * cdf
            slope = cdf + 0.5 * u * (1.0 - t * t) * (ROOT_2_PI * (1.0 + 3.0 * CUBIC * square))
            gates[p, rows, :width] = (d * v * slope).astype(BF16)
            gates[p, rows, width:] = (d * act).astype(BF16)
            hidden[p, rows] = (act * v * w).astype(BF16)
        return 0

    lax.fori_loop(0, 8, part, 0)
    dims = (((0,), (0,)), ((), ()))
    both = lax.dot_general(
        cols[0].reshape(1024, 256), gates[...].reshape(1024, 2 * width), dims, preferred_element_type=F32
    )
    total[:, 0] = both[:, :width].reshape(8, 32, width)
    total[:, 1] = both[:, width:].reshape(8, 32, width)
    total[:, 2] = lax.dot_general(
        cols[1].reshape(1024, 256), hidden[...].reshape(1024, width), dims, preferred_element_type=F32
    ).reshape(8, 32, width)
    odd = z & 1
    near = jnp.where(odd == 1, z + 1, z - 1) & 7
    near = jnp.where(c == 0, z ^ 1, near)
    for k in range(4):
        keep[k] = total[((z >> 1) + k & 3) * 2 + odd]
        send[k] = total[((near >> 1) + k & 3) * 2 + (1 - odd)].astype(BF16)


def all_steps(tokens, grad_out, w_gate, w_lin, w_out_t, code, decode, stragglers):
    own = message(code, decode, stragglers, tokens, grad_out)
    row = [own]
    for k in (1, 2, 3):
        row.append(across(own, k, True))
    w_in, w_out = loaded_weights(w_gate, w_lin, w_out_t)
    row = jnp.stack(row)
    near = {}
    for k in (1, 3):
        near[k] = across(row, k, False)
    swap = sibling(row)
    rows = line_rows(row, swap)
    got = []
    for j in (1, 3):
        got.append(z_shift(rows, j))
    partial = part_of_line(rows, *got)
    partials = [partial, swapped(partial, "xl", 2, 1)]
    terms = []
    for part in partials:
        terms += [part, sibling(part)]
    low = across(near[1][:2], 3, False)
    high = across(near[3][2:], 1, False)
    other = {}
    for k in (1, 3):
        other[k] = sibling(near[k])
    state = gathered(0, (row, swap), w_in, w_out, ())
    for m in (1, 3):
        state = gathered(m, (near[m], other[m]), w_in, w_out, state)
    state, low, high = lax.optimization_barrier((state, low, high))
    halves = [sibling(low), sibling(high)]
    state = gathered(2, (low, high), w_in, w_out, state)
    keeps, got = [], []
    for cut in range(2):
        state, keep, send = finished(cut, halves, w_in, w_out, state, terms)
        keeps.append(keep)
        got.append(z_pair(send))
    results = []
    for cut in range(2):
        mixed = keeps[cut] + got[cut].astype(F32)
        sends = mixed.astype(BF16)
        if cut == 0:
            sends, keeps[1] = lax.optimization_barrier((sends, keeps[1]))
        result = mixed[0]
        for k in (2, 1, 3):
            result = result + z_step(sends[k], 2 * k).astype(F32)
        results.append(result)
    return jnp.transpose(jnp.concatenate(results, axis=2), (1, 0, 2))


def solution(mesh):
    split = Mesh(mesh.devices.reshape(2, 4, 8, 2, 2), ("xl", "y", "z", "xh", "c"))
    mp = ("xh", "c")
    in_specs = (P(BLK, mp), P(BLK, mp), P(None, mp), P(None, mp), P(None, mp), P(BLK, None), P(BLK), P())
    return jax.shard_map(all_steps, mesh=split, in_specs=in_specs, out_specs=P(BLK, None, mp), check_vma=False)
```

```python
import jax
import jax.numpy as jnp
from jax import lax
from jax.experimental import pallas as pl
from jax.experimental.pallas import tpu as pltpu
from jax.sharding import Mesh, PartitionSpec as P


BF16 = jnp.bfloat16
F32 = jnp.float32
I32 = jnp.int32
ROOT_2_PI = 0.7978845608028654
CUBIC = 0.044715
CUTS = ((0, 256), (256, 640))
OWN, EARLY, LATE, FAR = ((0, 0), (0, 1)), ((1, 0), (3, 1)), ((1, 1), (3, 0)), ((2, 0), (2, 1))
BLK = ("xl", "y", "z")
PLANE = ("xl", "y", "xh", "c")
SMEM = pl.BlockSpec(memory_space=pltpu.SMEM)
VMEM = pl.BlockSpec(memory_space=pltpu.VMEM)
PARAMS = pltpu.CompilerParams(vmem_limit_bytes=16 * 1024 * 1024)


def place():
    return [lax.axis_index(a).astype(I32) for a in ("xl", "y", "z", "xh", "c")]


def across(block, flip, first):
    route = []
    for xl in range(2):
        for y in range(4):
            for xh in range(2):
                for c in range(2):
                    on_x = (c == 0) == first
                    to = (xl ^ (flip & 1), y, xh ^ (flip >> 1), c) if on_x else (xl, y ^ flip, xh, c)
                    number = lambda a: ((a[0] * 4 + a[1]) * 2 + a[2]) * 2 + a[3]
                    route.append((number((xl, y, xh, c)), number(to)))
    return lax.ppermute(block, PLANE, route)


def swapped(block, axis, size, flip):
    return lax.ppermute(block, axis, [(i, i ^ flip) for i in range(size)])


def sibling(block):
    return lax.ppermute(block, "c", [(0, 1), (1, 0)])


def partner_of(z, c):
    return z ^ 1 if c == 0 else ((z + 1) % 8 if z % 2 else (z - 1) % 8)


def z_pair(block):
    return lax.ppermute(block, ("z", "c"), [(z * 2 + c, partner_of(z, c) * 2 + c) for z in range(8) for c in range(2)])


def z_shift(block, step):
    return lax.ppermute(
        block, ("z", "c"), [(z * 2 + c, (z + step + c) % 8 * 2 + c) for z in range(8) for c in range(2)]
    )


def z_step(block, step):
    return lax.ppermute(block, "z", [(z, (z + step) % 8) for z in range(8)])


def hbm(array):
    return pltpu.with_memory_space_constraint(array, pltpu.HBM)


def message_kernel(decode, code_in, stragglers_in, tokens, grad_out, out, code, stragglers, sems):
    pairs = (
        (tokens, out.at[pl.ds(0, 128)]),
        (grad_out, out.at[pl.ds(128, 128)]),
        (code_in, code),
        (stragglers_in, stragglers),
    )
    copies = [pltpu.make_async_copy(source, target, sems.at[i]) for i, (source, target) in enumerate(pairs)]
    for copy in copies:
        copy.start()
    for copy in copies[2:]:
        copy.wait()
    xl, y, z, _, _ = place()
    device = (xl * 4 + y) * 8 + z
    alive = stragglers[0] != device
    for i in range(1, 4):
        alive = alive & (stragglers[i] != device)
    scale = jnp.where(alive, decode[0], 0.0)
    lane = lax.broadcasted_iota(I32, (8, 128), 1)
    row = lax.broadcasted_iota(I32, (8, 128), 0)
    value = jnp.zeros((8, 128), F32)
    for j in range(5):
        value = jnp.where(lane == j, scale * code[0, j], value)
    high = value.astype(BF16).astype(F32)
    rest = value - high
    middle = rest.astype(BF16).astype(F32)
    low = rest - middle
    pieces = jnp.where(row == 0, high, jnp.where(row == 1, middle, jnp.where(row == 2, low, 0.0)))
    out[256:264, :] = jnp.zeros((8, 512), BF16)
    out[256:264, 0:128] = pieces.astype(BF16)
    for copy in copies[:2]:
        copy.wait()


def message(code, decode, stragglers, tokens, grad_out):
    return pl.pallas_call(
        message_kernel,
        out_shape=jax.ShapeDtypeStruct((264, 512), BF16),
        in_specs=[SMEM] + [pl.BlockSpec(memory_space=pltpu.HBM)] * 4,
        out_specs=VMEM,
        scratch_shapes=[pltpu.SMEM((1, 5), F32), pltpu.SMEM((4,), I32), pltpu.SemaphoreType.DMA((4,))],
        compiler_params=PARAMS,
        name="message",
    )(decode, *[hbm(a) for a in (code, stragglers, tokens, grad_out)])


def weights_kernel(w_gate, w_lin, w_out_t, w_in, w_out, sems):
    pairs = [(w_out_t, w_out)]
    for lower, upper in CUTS:
        width = upper - lower
        for n, w in enumerate((w_gate, w_lin)):
            target = w_in.at[:, :, pl.ds(2 * lower + n * width, width)]
            pairs.append((w.at[:, :, pl.ds(lower, width)], target))
    copies = [pltpu.make_async_copy(*pair, sems.at[i]) for i, pair in enumerate(pairs)]
    for copy in copies:
        copy.start()
    for copy in copies:
        copy.wait()


def loaded_weights(w_gate, w_lin, w_out_t):
    return pl.pallas_call(
        weights_kernel,
        out_shape=(
            jax.ShapeDtypeStruct((4, 512, 1280), BF16),
            jax.ShapeDtypeStruct((4, 512, 640), BF16),
        ),
        in_specs=[pl.BlockSpec(memory_space=pltpu.HBM)] * 3,
        out_specs=(VMEM, VMEM),
        scratch_shapes=[pltpu.SemaphoreType.DMA((5,))],
        compiler_params=PARAMS,
        name="load",
    )(*[hbm(w.reshape(4, 512, 640)) for w in (w_gate, w_lin, w_out_t)])


def rows_kernel(own_low, own_high, other_low, other_high, rows):
    c = lax.axis_index("c").astype(I32)
    rows[...] = jnp.zeros_like(rows)
    for dy in range(4):
        pair = (own_low, other_low) if dy < 2 else (own_high, other_high)
        piece = [block[dy % 2, 256:264, 0:128].astype(F32) for block in pair]
        piece = jnp.where(c == 1, piece[0], piece[1])
        rows[dy : dy + 1, :] = jnp.sum(piece, axis=0, keepdims=True)


def line_rows(*blocks):
    return pl.pallas_call(
        rows_kernel,
        out_shape=jax.ShapeDtypeStruct((8, 128), F32),
        in_specs=[VMEM] * 4,
        out_specs=VMEM,
        compiler_params=PARAMS,
        name="rows",
    )(*blocks)


def part_kernel(rows, near, far, out):
    c = lax.axis_index("c").astype(I32)
    lane = lax.broadcasted_iota(I32, (8, 128), 1)
    total = jnp.where((lane == 0) & (c == 0), rows[...], 0.0)
    total = jnp.where(lane == 1 + c, near[...], total)
    out[...] = jnp.where(lane == 3 + c, far[...], total)


def part_of_line(*rows):
    return pl.pallas_call(
        part_kernel,
        out_shape=jax.ShapeDtypeStruct((8, 128), F32),
        in_specs=[VMEM] * 3,
        out_specs=VMEM,
        compiler_params=PARAMS,
        name="part",
    )(*rows)


def add_block(m, j, ec, block, w_in, w_out, acc, cols, cuts=CUTS, with_cols=True):
    xl, y, _, xh, c = place()
    x_first = (c ^ ec) == 0
    eh = jnp.where(x_first, j, m >> 1)
    p0 = jnp.where(x_first, 2 * m, 4 * j + (m & 1))
    p1 = jnp.where(x_first, 2 * m + 1, 4 * j + 2 + (m & 1))
    shard = (xh ^ eh) * 2 + (c ^ ec)
    xs = block[:, 0:128].reshape(256, 512)
    ys = block[:, 128:256].reshape(256, 512)
    first, end = cuts[0][0], cuts[-1][1]
    pre = jnp.dot(xs, w_in[shard, :, 2 * first : 2 * end], preferred_element_type=F32)
    for lower, upper in cuts:
        width = upper - lower
        for n in range(2):
            at = 2 * (lower - first) + n * width
            acc[n, p0, :, lower:upper] += pre[:128, at : at + width]
            acc[n, p1, :, lower:upper] += pre[128:, at : at + width]
    dh = jnp.dot(ys, w_out[shard, :, first:end], preferred_element_type=F32)
    acc[2, p0, :, first:end] += dh[:128]
    acc[2, p1, :, first:end] += dh[128:]
    if not with_cols:
        return

    @pl.when((ec == ((y >> 1) ^ c)) & (eh == (xl ^ xh)))
    def _():
        low = (y & 1) == 0
        for n, v in ((0, xs), (1, ys)):
            v = jnp.where(low, v[:, :256], v[:, 256:])
            cols[n, p0] = v[:128]
            cols[n, p1] = v[128:]


STATE = (jax.ShapeDtypeStruct((3, 8, 128, 640), F32), jax.ShapeDtypeStruct((2, 8, 128, 256), BF16))


def priced(giga):
    return pl.CostEstimate(flops=giga << 30, bytes_accessed=1 << 20, transcendentals=0)


def gathered(items, w_in, w_out, state):
    n = len(items)

    def kernel(*refs):
        blocks, (w_in, w_out), (acc, cols) = refs[:n], refs[n : n + 2], refs[-2:]
        if not state:
            acc[...] = jnp.zeros_like(acc)
        for (m, j, ec, _), block in zip(items, blocks):
            add_block(m, j, ec, block, w_in, w_out, acc, cols)

    return pl.pallas_call(
        kernel,
        out_shape=STATE,
        in_specs=[VMEM] * (n + 2 + len(state)),
        out_specs=(VMEM, VMEM),
        input_output_aliases={n + 2: 0, n + 3: 1} if state else {},
        compiler_params=PARAMS,
        cost_estimate=priced(n // 2),
    )(*[item[3] for item in items], w_in, w_out, *state)


def finished(cut, items, w_in, w_out, state, terms):
    width = CUTS[cut][1] - CUTS[cut][0]

    def kernel(*refs):
        blocks, (w_in, w_out), terms = refs[:2], refs[2:4], refs[6:10]
        acc, cols, *rest = refs[10:]
        for (m, j, ec, _), block in zip(items, blocks):
            add_block(m, j, ec, block, w_in, w_out, acc, cols, (CUTS[cut],), cut == 0)
        last_kernel(CUTS[cut], terms, acc, cols, *rest)

    *state, keep, send = pl.pallas_call(
        kernel,
        out_shape=STATE
        + (jax.ShapeDtypeStruct((4, 3, 32, width), F32), jax.ShapeDtypeStruct((4, 3, 32, width), BF16)),
        in_specs=[VMEM] * 10,
        out_specs=(VMEM,) * 4,
        input_output_aliases={4: 0, 5: 1},
        scratch_shapes=[
            pltpu.VMEM((8, 128, 2 * width), BF16),
            pltpu.VMEM((8, 128, width), BF16),
            pltpu.VMEM((8, 3, 32, width), F32),
        ],
        compiler_params=PARAMS,
        cost_estimate=priced(2),
    )(*[item[3] for item in items], w_in, w_out, *state, *terms)
    return state, keep, send


def last_kernel(cut, terms, acc, cols, keep, send, gates, hidden, total):
    xl, y, z, _, c = place()
    lane = lax.broadcasted_iota(I32, (8, 128), 1)
    lower, upper = cut
    width = upper - lower
    row = lax.broadcasted_iota(I32, (8, 128), 0)
    known = (lane < 5) & (row < 4)
    workers = [(((xl ^ ex) * 4 + (y ^ row)) & 7) * 8 + ((z - lane) & 7) for ex in range(2)]

    def part(p, _):
        dy, ex = p >> 1, p & 1
        number = ((xl ^ ex) * 4 + (y ^ dy)) * 8 + z
        w = F32(0.0)
        for i, worker in enumerate(workers):
            mine = known & (((number - lane) & 63) == worker)
            w = w + jnp.sum(jnp.where(mine, terms[2 * i][...] + terms[2 * i + 1][...], 0.0))
        for r in range(0, 128, 32):
            rows = pl.ds(r, 32)
            u = acc[0, p, rows, lower:upper]
            v = acc[1, p, rows, lower:upper]
            d = acc[2, p, rows, lower:upper] * w
            square = u * u
            t = jnp.tanh(ROOT_2_PI * (u + CUBIC * (square * u)))
            cdf = 0.5 * (1.0 + t)
            act = u * cdf
            slope = cdf + 0.5 * u * (1.0 - t * t) * (ROOT_2_PI * (1.0 + 3.0 * CUBIC * square))
            gates[p, rows, :width] = (d * v * slope).astype(BF16)
            gates[p, rows, width:] = (d * act).astype(BF16)
            hidden[p, rows] = (act * v * w).astype(BF16)
        return 0

    lax.fori_loop(0, 8, part, 0)
    dims = (((0,), (0,)), ((), ()))
    both = lax.dot_general(
        cols[0].reshape(1024, 256), gates[...].reshape(1024, 2 * width), dims, preferred_element_type=F32
    )
    total[:, 0] = both[:, :width].reshape(8, 32, width)
    total[:, 1] = both[:, width:].reshape(8, 32, width)
    total[:, 2] = lax.dot_general(
        cols[1].reshape(1024, 256), hidden[...].reshape(1024, width), dims, preferred_element_type=F32
    ).reshape(8, 32, width)
    odd = z & 1
    near = jnp.where(odd == 1, z + 1, z - 1) & 7
    near = jnp.where(c == 0, z ^ 1, near)
    for k in range(4):
        keep[k] = total[((z >> 1) + k & 3) * 2 + odd]
        send[k] = total[((near >> 1) + k & 3) * 2 + (1 - odd)].astype(BF16)


def all_steps(tokens, grad_out, w_gate, w_lin, w_out_t, code, decode, stragglers):
    own = message(code, decode, stragglers, tokens, grad_out)
    first = {}
    for k in (1, 2, 3):
        first[k] = across(own, k, True)
    w_in, w_out = loaded_weights(w_gate, w_lin, w_out_t)
    blocks = {(0, 0): jnp.stack([own, first[1]]), (0, 1): jnp.stack([first[2], first[3]])}
    others = {}
    for k, j in EARLY + LATE:
        blocks[k, j] = across(blocks[0, j], k, False)
    for j, came in ((0, 1), (1, 3)):
        blocks[2, j] = across(blocks[came, j], came ^ 2, False)
    for k, j in OWN + EARLY + LATE:
        others[k, j] = sibling(blocks[k, j])
    rows = line_rows(blocks[0, 0], blocks[0, 1], others[0, 0], others[0, 1])
    got = []
    for j in (1, 3):
        got.append(z_shift(rows, j))
    partial = part_of_line(rows, *got)
    partials = [partial, swapped(partial, "xl", 2, 1)]
    terms = []
    for part in partials:
        terms += [part, sibling(part)]

    def items(keys, sides=(0, 1)):
        return [(m, j, ec, (blocks, others)[ec][m, j]) for m, j in keys for ec in sides]

    state = ()
    for keys in (OWN, EARLY, LATE):
        state = gathered(items(keys), w_in, w_out, state)
    state, blocks[2, 0], blocks[2, 1] = lax.optimization_barrier((state, blocks[2, 0], blocks[2, 1]))
    for k, j in FAR:
        others[k, j] = sibling(blocks[k, j])
    state = gathered(items(FAR, (0,)), w_in, w_out, state)
    halves = items(FAR, (1,))
    keeps, got = [], []
    for cut in range(2):
        state, keep, send = finished(cut, halves, w_in, w_out, state, terms)
        keeps.append(keep)
        got.append(z_pair(send))
    results = []
    for cut in range(2):
        mixed = keeps[cut] + got[cut].astype(F32)
        sends = mixed.astype(BF16)
        if cut == 0:
            sends, keeps[1] = lax.optimization_barrier((sends, keeps[1]))
        result = mixed[0]
        for k in (2, 1, 3):
            result = result + z_step(sends[k], 2 * k).astype(F32)
        results.append(result)
    return jnp.transpose(jnp.concatenate(results, axis=2), (1, 0, 2))


def solution(mesh):
    split = Mesh(mesh.devices.reshape(2, 4, 8, 2, 2), ("xl", "y", "z", "xh", "c"))
    mp = ("xh", "c")
    in_specs = (P(BLK, mp), P(BLK, mp), P(None, mp), P(None, mp), P(None, mp), P(BLK, None), P(BLK), P())
    return jax.shard_map(all_steps, mesh=split, in_specs=in_specs, out_specs=P(BLK, None, mp), check_vma=False)
```

```python
import jax
import jax.numpy as jnp
from jax import lax
from jax.experimental import pallas as pl
from jax.experimental.pallas import tpu as pltpu
from jax.sharding import Mesh, PartitionSpec as P


BF16 = jnp.bfloat16
F32 = jnp.float32
I32 = jnp.int32
ROOT_2_PI = 0.7978845608028654
CUBIC = 0.044715
CUTS = ((0, 256), (256, 640))
OWN, EARLY, LATE, FAR = ((0, 0), (0, 1)), ((1, 0), (3, 1)), ((1, 1), (3, 0)), ((2, 0), (2, 1))
BLK = ("xl", "y", "z")
PLANE = ("xl", "y", "xh", "c")
SMEM = pl.BlockSpec(memory_space=pltpu.SMEM)
VMEM = pl.BlockSpec(memory_space=pltpu.VMEM)
PARAMS = pltpu.CompilerParams(vmem_limit_bytes=16 * 1024 * 1024)


def place():
    return [lax.axis_index(a).astype(I32) for a in ("xl", "y", "z", "xh", "c")]


def across(block, flip, first):
    route = []
    for xl in range(2):
        for y in range(4):
            for xh in range(2):
                for c in range(2):
                    on_x = (c == 0) == first
                    to = (xl ^ (flip & 1), y, xh ^ (flip >> 1), c) if on_x else (xl, y ^ flip, xh, c)
                    number = lambda a: ((a[0] * 4 + a[1]) * 2 + a[2]) * 2 + a[3]
                    route.append((number((xl, y, xh, c)), number(to)))
    return lax.ppermute(block, PLANE, route)


def swapped(block, axis, size, flip):
    return lax.ppermute(block, axis, [(i, i ^ flip) for i in range(size)])


def sibling(block):
    return lax.ppermute(block, "c", [(0, 1), (1, 0)])


def partner_of(z, c):
    return z ^ 1 if c == 0 else ((z + 1) % 8 if z % 2 else (z - 1) % 8)


def z_pair(block):
    return lax.ppermute(block, ("z", "c"), [(z * 2 + c, partner_of(z, c) * 2 + c) for z in range(8) for c in range(2)])


def z_shift(block, step):
    return lax.ppermute(
        block, ("z", "c"), [(z * 2 + c, (z + step + c) % 8 * 2 + c) for z in range(8) for c in range(2)]
    )


def z_step(block, step):
    return lax.ppermute(block, "z", [(z, (z + step) % 8) for z in range(8)])


def hbm(array):
    return pltpu.with_memory_space_constraint(array, pltpu.HBM)


def message_kernel(decode, code_in, stragglers_in, tokens, grad_out, out, code, stragglers, sems):
    pairs = (
        (tokens, out.at[pl.ds(0, 128)]),
        (grad_out, out.at[pl.ds(128, 128)]),
        (code_in, code),
        (stragglers_in, stragglers),
    )
    copies = [pltpu.make_async_copy(source, target, sems.at[i]) for i, (source, target) in enumerate(pairs)]
    for copy in copies:
        copy.start()
    for copy in copies[2:]:
        copy.wait()
    xl, y, z, _, _ = place()
    device = (xl * 4 + y) * 8 + z
    alive = stragglers[0] != device
    for i in range(1, 4):
        alive = alive & (stragglers[i] != device)
    scale = jnp.where(alive, decode[0], 0.0)
    lane = lax.broadcasted_iota(I32, (8, 128), 1)
    row = lax.broadcasted_iota(I32, (8, 128), 0)
    value = jnp.zeros((8, 128), F32)
    for j in range(5):
        value = jnp.where(lane == j, scale * code[0, j], value)
    high = value.astype(BF16).astype(F32)
    rest = value - high
    middle = rest.astype(BF16).astype(F32)
    low = rest - middle
    pieces = jnp.where(row == 0, high, jnp.where(row == 1, middle, jnp.where(row == 2, low, 0.0)))
    out[256:264, :] = jnp.zeros((8, 512), BF16)
    out[256:264, 0:128] = pieces.astype(BF16)
    for copy in copies[:2]:
        copy.wait()


def message(code, decode, stragglers, tokens, grad_out):
    return pl.pallas_call(
        message_kernel,
        out_shape=jax.ShapeDtypeStruct((264, 512), BF16),
        in_specs=[SMEM] + [pl.BlockSpec(memory_space=pltpu.HBM)] * 4,
        out_specs=VMEM,
        scratch_shapes=[pltpu.SMEM((1, 5), F32), pltpu.SMEM((4,), I32), pltpu.SemaphoreType.DMA((4,))],
        compiler_params=PARAMS,
        name="message",
    )(decode, *[hbm(a) for a in (code, stragglers, tokens, grad_out)])


def weights_kernel(w_gate, w_lin, w_out_t, w_in, w_out, sems):
    pairs = [(w_out_t, w_out)]
    for lower, upper in CUTS:
        width = upper - lower
        for n, w in enumerate((w_gate, w_lin)):
            target = w_in.at[:, :, pl.ds(2 * lower + n * width, width)]
            pairs.append((w.at[:, :, pl.ds(lower, width)], target))
    copies = [pltpu.make_async_copy(*pair, sems.at[i]) for i, pair in enumerate(pairs)]
    for copy in copies:
        copy.start()
    for copy in copies:
        copy.wait()


def loaded_weights(w_gate, w_lin, w_out_t):
    return pl.pallas_call(
        weights_kernel,
        out_shape=(
            jax.ShapeDtypeStruct((4, 512, 1280), BF16),
            jax.ShapeDtypeStruct((4, 512, 640), BF16),
        ),
        in_specs=[pl.BlockSpec(memory_space=pltpu.HBM)] * 3,
        out_specs=(VMEM, VMEM),
        scratch_shapes=[pltpu.SemaphoreType.DMA((5,))],
        compiler_params=PARAMS,
        name="load",
    )(*[hbm(w.reshape(4, 512, 640)) for w in (w_gate, w_lin, w_out_t)])


def rows_kernel(own_low, own_high, other_low, other_high, rows):
    c = lax.axis_index("c").astype(I32)
    rows[...] = jnp.zeros_like(rows)
    for dy in range(4):
        pair = (own_low, other_low) if dy < 2 else (own_high, other_high)
        piece = [block[dy % 2, 256:264, 0:128].astype(F32) for block in pair]
        piece = jnp.where(c == 1, piece[0], piece[1])
        rows[dy : dy + 1, :] = jnp.sum(piece, axis=0, keepdims=True)


def line_rows(*blocks):
    return pl.pallas_call(
        rows_kernel,
        out_shape=jax.ShapeDtypeStruct((8, 128), F32),
        in_specs=[VMEM] * 4,
        out_specs=VMEM,
        compiler_params=PARAMS,
        name="rows",
    )(*blocks)


def part_kernel(rows, near, far, out):
    c = lax.axis_index("c").astype(I32)
    lane = lax.broadcasted_iota(I32, (8, 128), 1)
    total = jnp.where((lane == 0) & (c == 0), rows[...], 0.0)
    total = jnp.where(lane == 1 + c, near[...], total)
    out[...] = jnp.where(lane == 3 + c, far[...], total)


def part_of_line(*rows):
    return pl.pallas_call(
        part_kernel,
        out_shape=jax.ShapeDtypeStruct((8, 128), F32),
        in_specs=[VMEM] * 3,
        out_specs=VMEM,
        compiler_params=PARAMS,
        name="part",
    )(*rows)


def add_block(m, j, ec, block, w_in, w_out, acc, cols, cuts=CUTS, with_cols=True):
    xl, y, _, xh, c = place()
    x_first = (c ^ ec) == 0
    eh = jnp.where(x_first, j, m >> 1)
    p0 = jnp.where(x_first, 2 * m, 4 * j + (m & 1))
    p1 = jnp.where(x_first, 2 * m + 1, 4 * j + 2 + (m & 1))
    shard = (xh ^ eh) * 2 + (c ^ ec)
    xs = block[:, 0:128].reshape(256, 512)
    ys = block[:, 128:256].reshape(256, 512)
    first, end = cuts[0][0], cuts[-1][1]
    pre = jnp.dot(xs, w_in[shard, :, 2 * first : 2 * end], preferred_element_type=F32)
    for lower, upper in cuts:
        width = upper - lower
        for n in range(2):
            at = 2 * (lower - first) + n * width
            acc[n, p0, :, lower:upper] += pre[:128, at : at + width]
            acc[n, p1, :, lower:upper] += pre[128:, at : at + width]
    dh = jnp.dot(ys, w_out[shard, :, first:end], preferred_element_type=F32)
    acc[2, p0, :, first:end] += dh[:128]
    acc[2, p1, :, first:end] += dh[128:]
    if not with_cols:
        return

    @pl.when((ec == ((y >> 1) ^ c)) & (eh == (xl ^ xh)))
    def _():
        low = (y & 1) == 0
        for n, v in ((0, xs), (1, ys)):
            v = jnp.where(low, v[:, :256], v[:, 256:])
            cols[n, p0] = v[:128]
            cols[n, p1] = v[128:]


STATE = (jax.ShapeDtypeStruct((3, 8, 128, 640), F32), jax.ShapeDtypeStruct((2, 8, 128, 256), BF16))


def priced(giga):
    return pl.CostEstimate(flops=giga << 30, bytes_accessed=1 << 20, transcendentals=0)


def gathered(items, w_in, w_out, state):
    n = len(items)

    def kernel(*refs):
        blocks, (w_in, w_out), (acc, cols) = refs[:n], refs[n : n + 2], refs[-2:]
        if not state:
            acc[...] = jnp.zeros_like(acc)
        for (m, j, ec, _), block in zip(items, blocks):
            add_block(m, j, ec, block, w_in, w_out, acc, cols)

    return pl.pallas_call(
        kernel,
        out_shape=STATE,
        in_specs=[VMEM] * (n + 2 + len(state)),
        out_specs=(VMEM, VMEM),
        input_output_aliases={n + 2: 0, n + 3: 1} if state else {},
        compiler_params=PARAMS,
        cost_estimate=priced(n // 2),
    )(*[item[3] for item in items], w_in, w_out, *state)


def finished(cut, items, w_in, w_out, state, terms):
    width = CUTS[cut][1] - CUTS[cut][0]

    def kernel(*refs):
        blocks, (w_in, w_out), terms = refs[:2], refs[2:4], refs[6:10]
        acc, cols, *rest = refs[10:]
        for (m, j, ec, _), block in zip(items, blocks):
            add_block(m, j, ec, block, w_in, w_out, acc, cols, (CUTS[cut],), cut == 0)
        last_kernel(CUTS[cut], terms, acc, cols, *rest)

    *state, keep, send = pl.pallas_call(
        kernel,
        out_shape=STATE
        + (jax.ShapeDtypeStruct((4, 3, 32, width), F32), jax.ShapeDtypeStruct((4, 3, 32, width), BF16)),
        in_specs=[VMEM] * 10,
        out_specs=(VMEM,) * 4,
        input_output_aliases={4: 0, 5: 1},
        scratch_shapes=[
            pltpu.VMEM((8, 128, 2 * width), BF16),
            pltpu.VMEM((8, 128, width), BF16),
            pltpu.VMEM((8, 3, 32, width), F32),
        ],
        compiler_params=PARAMS,
        cost_estimate=priced(2),
    )(*[item[3] for item in items], w_in, w_out, *state, *terms)
    return state, keep, send


def last_kernel(cut, terms, acc, cols, keep, send, gates, hidden, total):
    xl, y, z, _, c = place()
    lane = lax.broadcasted_iota(I32, (8, 128), 1)
    lower, upper = cut
    width = upper - lower
    row = lax.broadcasted_iota(I32, (8, 128), 0)
    known = (lane < 5) & (row < 4)
    workers = [(((xl ^ ex) * 4 + (y ^ row)) & 7) * 8 + ((z - lane) & 7) for ex in range(2)]

    def part(p, _):
        dy, ex = p >> 1, p & 1
        number = ((xl ^ ex) * 4 + (y ^ dy)) * 8 + z
        w = F32(0.0)
        for i, worker in enumerate(workers):
            mine = known & (((number - lane) & 63) == worker)
            w = w + jnp.sum(jnp.where(mine, terms[2 * i][...] + terms[2 * i + 1][...], 0.0))
        for r in range(0, 128, 32):
            rows = pl.ds(r, 32)
            u = acc[0, p, rows, lower:upper]
            v = acc[1, p, rows, lower:upper]
            d = acc[2, p, rows, lower:upper] * w
            square = u * u
            t = jnp.tanh(ROOT_2_PI * (u + CUBIC * (square * u)))
            cdf = 0.5 * (1.0 + t)
            act = u * cdf
            slope = cdf + 0.5 * u * (1.0 - t * t) * (ROOT_2_PI * (1.0 + 3.0 * CUBIC * square))
            gates[p, rows, :width] = (d * v * slope).astype(BF16)
            gates[p, rows, width:] = (d * act).astype(BF16)
            hidden[p, rows] = (act * v * w).astype(BF16)
        return 0

    lax.fori_loop(0, 8, part, 0)
    dims = (((0,), (0,)), ((), ()))
    both = lax.dot_general(
        cols[0].reshape(1024, 256), gates[...].reshape(1024, 2 * width), dims, preferred_element_type=F32
    )
    total[:, 0] = both[:, :width].reshape(8, 32, width)
    total[:, 1] = both[:, width:].reshape(8, 32, width)
    total[:, 2] = lax.dot_general(
        cols[1].reshape(1024, 256), hidden[...].reshape(1024, width), dims, preferred_element_type=F32
    ).reshape(8, 32, width)
    odd = z & 1
    near = jnp.where(odd == 1, z + 1, z - 1) & 7
    near = jnp.where(c == 0, z ^ 1, near)
    for k in range(4):
        keep[k] = total[((z >> 1) + k & 3) * 2 + odd]
        send[k] = total[((near >> 1) + k & 3) * 2 + (1 - odd)].astype(BF16)


def all_steps(tokens, grad_out, w_gate, w_lin, w_out_t, code, decode, stragglers):
    own = message(code, decode, stragglers, tokens, grad_out)
    first = {}
    for k in (1, 2, 3):
        first[k] = across(own, k, True)
    w_in, w_out = loaded_weights(w_gate, w_lin, w_out_t)
    blocks = {(0, 0): jnp.stack([own, first[1]]), (0, 1): jnp.stack([first[2], first[3]])}
    others = {}
    for k, j in EARLY + LATE:
        blocks[k, j] = across(blocks[0, j], k, False)
    for j, came in ((0, 1), (1, 3)):
        blocks[2, j] = across(blocks[came, j], came ^ 2, False)
    for k, j in OWN + EARLY + LATE:
        others[k, j] = sibling(blocks[k, j])
    rows = line_rows(blocks[0, 0], blocks[0, 1], others[0, 0], others[0, 1])
    got = []
    for j in (1, 3):
        got.append(z_shift(rows, j))
    partial = part_of_line(rows, *got)
    partials = [partial, swapped(partial, "xl", 2, 1)]
    terms = []
    for part in partials:
        terms += [part, sibling(part)]

    def items(keys, sides=(0, 1)):
        return [(m, j, ec, (blocks, others)[ec][m, j]) for m, j in keys for ec in sides]

    state = gathered(items(OWN), w_in, w_out, ())
    state = gathered(items(EARLY), w_in, w_out, state)
    state, blocks[2, 0], blocks[2, 1] = lax.optimization_barrier((state, blocks[2, 0], blocks[2, 1]))
    for k, j in FAR:
        others[k, j] = sibling(blocks[k, j])
    state = gathered(items(LATE), w_in, w_out, state)
    state = gathered(items(FAR, (0,)), w_in, w_out, state)
    halves = items(FAR, (1,))
    keeps, got = [], []
    for cut in range(2):
        state, keep, send = finished(cut, halves, w_in, w_out, state, terms)
        keeps.append(keep)
        got.append(z_pair(send))
    results, across_ring = [], []
    for cut in range(2):
        mixed = keeps[cut] + got[cut].astype(F32)
        sends = mixed.astype(BF16)
        if cut == 0:
            sends, keeps[1] = lax.optimization_barrier((sends, keeps[1]))
        across_ring.append(sends[2])
        result = mixed[0]
        for k in (1, 3):
            result = result + z_step(sends[k], 2 * k).astype(F32)
        results.append(result)
    opposite = z_step(jnp.concatenate(across_ring, axis=2), 4)
    return jnp.transpose(jnp.concatenate(results, axis=2) + opposite.astype(F32), (1, 0, 2))


def solution(mesh):
    split = Mesh(mesh.devices.reshape(2, 4, 8, 2, 2), ("xl", "y", "z", "xh", "c"))
    mp = ("xh", "c")
    in_specs = (P(BLK, mp), P(BLK, mp), P(None, mp), P(None, mp), P(None, mp), P(BLK, None), P(BLK), P())
    return jax.shard_map(all_steps, mesh=split, in_specs=in_specs, out_specs=P(BLK, None, mp), check_vma=False)
```

```python
from functools import partial as partial_call

import jax
import jax.numpy as jnp
from jax import lax
from jax.experimental import pallas as pl
from jax.experimental.pallas import tpu as pltpu
from jax.sharding import Mesh, PartitionSpec as P


BF16 = jnp.bfloat16
F32 = jnp.float32
I32 = jnp.int32
ROOT_2_PI = 0.7978845608028654
CUBIC = 0.044715
CUTS = ((0, 384), (384, 640))
OWN, EARLY, LATE, FAR = ((0, 0), (0, 1)), ((1, 0), (3, 1)), ((1, 1), (3, 0)), ((2, 0), (2, 1))
BLK = ("xl", "y", "z")
PLANE = ("xl", "y", "xh", "c")
SMEM = pl.BlockSpec(memory_space=pltpu.SMEM)
VMEM = pl.BlockSpec(memory_space=pltpu.VMEM)
PARAMS = pltpu.CompilerParams(vmem_limit_bytes=16 * 1024 * 1024)


def place():
    return [lax.axis_index(a).astype(I32) for a in ("xl", "y", "z", "xh", "c")]


def across(block, flip, first):
    route = []
    for xl in range(2):
        for y in range(4):
            for xh in range(2):
                for c in range(2):
                    on_x = (c == 0) == first
                    to = (xl ^ (flip & 1), y, xh ^ (flip >> 1), c) if on_x else (xl, y ^ flip, xh, c)
                    number = lambda a: ((a[0] * 4 + a[1]) * 2 + a[2]) * 2 + a[3]
                    route.append((number((xl, y, xh, c)), number(to)))
    return lax.ppermute(block, PLANE, route)


def swapped(block, axis, size, flip):
    return lax.ppermute(block, axis, [(i, i ^ flip) for i in range(size)])


def sibling(block):
    return lax.ppermute(block, "c", [(0, 1), (1, 0)])


def partner_of(z, c):
    return z ^ 1 if c == 0 else ((z + 1) % 8 if z % 2 else (z - 1) % 8)


def z_pair(block):
    return lax.ppermute(block, ("z", "c"), [(z * 2 + c, partner_of(z, c) * 2 + c) for z in range(8) for c in range(2)])


def z_shift(block, step):
    return lax.ppermute(
        block, ("z", "c"), [(z * 2 + c, (z + step + c) % 8 * 2 + c) for z in range(8) for c in range(2)]
    )


def z_step(block, step):
    return lax.ppermute(block, "z", [(z, (z + step) % 8) for z in range(8)])


def hbm(array):
    return pltpu.with_memory_space_constraint(array, pltpu.HBM)


def message_kernel(decode, code_in, stragglers_in, tokens, grad_out, out, code, stragglers, sems):
    pairs = (
        (tokens, out.at[pl.ds(0, 128)]),
        (grad_out, out.at[pl.ds(128, 128)]),
        (code_in, code),
        (stragglers_in, stragglers),
    )
    copies = [pltpu.make_async_copy(source, target, sems.at[i]) for i, (source, target) in enumerate(pairs)]
    for copy in copies:
        copy.start()
    for copy in copies[2:]:
        copy.wait()
    xl, y, z, _, _ = place()
    device = (xl * 4 + y) * 8 + z
    alive = stragglers[0] != device
    for i in range(1, 4):
        alive = alive & (stragglers[i] != device)
    scale = jnp.where(alive, decode[0], 0.0)
    lane = lax.broadcasted_iota(I32, (8, 128), 1)
    row = lax.broadcasted_iota(I32, (8, 128), 0)
    value = jnp.zeros((8, 128), F32)
    for j in range(5):
        value = jnp.where(lane == j, scale * code[0, j], value)
    high = value.astype(BF16).astype(F32)
    rest = value - high
    middle = rest.astype(BF16).astype(F32)
    low = rest - middle
    pieces = jnp.where(row == 0, high, jnp.where(row == 1, middle, jnp.where(row == 2, low, 0.0)))
    out[256:264, :] = jnp.zeros((8, 512), BF16)
    out[256:264, 0:128] = pieces.astype(BF16)
    for copy in copies[:2]:
        copy.wait()


def message(code, decode, stragglers, tokens, grad_out):
    return pl.pallas_call(
        message_kernel,
        out_shape=jax.ShapeDtypeStruct((264, 512), BF16),
        in_specs=[SMEM] + [pl.BlockSpec(memory_space=pltpu.HBM)] * 4,
        out_specs=VMEM,
        scratch_shapes=[pltpu.SMEM((1, 5), F32), pltpu.SMEM((4,), I32), pltpu.SemaphoreType.DMA((4,))],
        compiler_params=PARAMS,
        name="message",
    )(decode, *[hbm(a) for a in (code, stragglers, tokens, grad_out)])


def weights_kernel(w_gate, w_lin, w_out_t, w_in, w_out, sems):
    xh = lax.axis_index("xh").astype(I32)
    copies = []
    for side in range(2):
        for eh in range(2):
            source, target = 2 * (xh ^ eh) + side, pl.ds(512 * (2 * side + eh), 512)
            copies.append((w_out_t.at[source], w_out.at[target]))
            for lower, upper in CUTS:
                width = upper - lower
                for n, w in enumerate((w_gate, w_lin)):
                    columns = pl.ds(2 * lower + n * width, width)
                    copies.append((w.at[source, :, pl.ds(lower, width)], w_in.at[target, columns]))
    copies = [pltpu.make_async_copy(*pair, sems.at[i]) for i, pair in enumerate(copies)]
    for copy in copies:
        copy.start()
    for copy in copies:
        copy.wait()


def loaded_weights(w_gate, w_lin, w_out_t):
    return pl.pallas_call(
        weights_kernel,
        out_shape=(
            jax.ShapeDtypeStruct((2048, 1280), BF16),
            jax.ShapeDtypeStruct((2048, 640), BF16),
        ),
        in_specs=[pl.BlockSpec(memory_space=pltpu.HBM)] * 3,
        out_specs=(VMEM, VMEM),
        scratch_shapes=[pltpu.SemaphoreType.DMA((20,))],
        compiler_params=PARAMS,
        name="load",
    )(*[hbm(w.reshape(4, 512, 640)) for w in (w_gate, w_lin, w_out_t)])


def rows_kernel(own_low, own_high, other_low, other_high, rows):
    c = lax.axis_index("c").astype(I32)
    rows[...] = jnp.zeros_like(rows)
    for dy in range(4):
        pair = (own_low, other_low) if dy < 2 else (own_high, other_high)
        piece = [block[dy % 2, 256:264, 0:128].astype(F32) for block in pair]
        piece = jnp.where(c == 1, piece[0], piece[1])
        rows[dy : dy + 1, :] = jnp.sum(piece, axis=0, keepdims=True)


def line_rows(*blocks):
    return pl.pallas_call(
        rows_kernel,
        out_shape=jax.ShapeDtypeStruct((8, 128), F32),
        in_specs=[VMEM] * 4,
        out_specs=VMEM,
        compiler_params=PARAMS,
        name="rows",
    )(*blocks)


def part_kernel(rows, near, far, out):
    c = lax.axis_index("c").astype(I32)
    lane = lax.broadcasted_iota(I32, (8, 128), 1)
    total = jnp.where((lane == 0) & (c == 0), rows[...], 0.0)
    total = jnp.where(lane == 1 + c, near[...], total)
    out[...] = jnp.where(lane == 3 + c, far[...], total)


def part_of_line(*rows):
    return pl.pallas_call(
        part_kernel,
        out_shape=jax.ShapeDtypeStruct((8, 128), F32),
        in_specs=[VMEM] * 3,
        out_specs=VMEM,
        compiler_params=PARAMS,
        name="part",
    )(*rows)


def sides(own, other):
    c = lax.axis_index("c").astype(I32)
    pairs = [(mine[...], theirs[...]) for mine, theirs in zip(own, other)]
    x_first = [jnp.where(c == 0, mine, theirs) for mine, theirs in pairs]
    y_first = [jnp.where(c == 0, theirs, mine) for mine, theirs in pairs]
    return x_first, y_first


def add_rows(side, ehs, rows, blocks, w_in, w_out, acc, cols, stored=(), cuts=CUTS):
    xl, y, _, xh, _ = place()
    low, end = 1024 * side + 512 * ehs[0], 1024 * side + 512 * (ehs[-1] + 1)
    parts = []
    for n in range(2):
        pieces = [[b[:, 128 * n : 128 * n + 128].reshape(256, 512) for b in row] for row in blocks]
        parts.append(jnp.concatenate([jnp.concatenate(p, axis=1) for p in pieces], axis=0))
    first, last = cuts[0][0], cuts[-1][1]
    pre = jnp.dot(parts[0], w_in[low:end, 2 * first : 2 * last], preferred_element_type=F32)
    dh = jnp.dot(parts[1], w_out[low:end, first:last], preferred_element_type=F32)
    for i, p in enumerate(rows):
        at_rows = slice(128 * i, 128 * i + 128)
        values = [(2, first, last, dh[at_rows])]
        for lower, upper in cuts:
            for n in range(2):
                at = 2 * (lower - first) + n * (upper - lower)
                values.append((n, lower, upper, pre[at_rows, at : at + upper - lower]))
        for n, lower, upper, value in values:
            if p in stored:
                acc[n, p, :, lower:upper] = value
            else:
                acc[n, p, :, lower:upper] += value
    if cols is None:
        return
    for k, eh in enumerate(ehs):

        @pl.when(((y >> 1) == side) & ((xl ^ xh) == eh))
        def _():
            for n in range(2):
                v = parts[n][:, 512 * k : 512 * k + 512]
                v = jnp.where((y & 1) == 0, v[:, :256], v[:, 256:])
                for i, p in enumerate(rows):
                    cols[n, p] = v[128 * i : 128 * i + 128]


def first_kernel(own0, own1, other0, other1, w_in, w_out, acc, cols):
    (a0, a1), (b0, b1) = sides((own0, own1), (other0, other1))
    for p in (3, 5, 7):
        acc[:, p] = jnp.zeros((3, 128, 640), F32)
    add_rows(1, (0,), (0, 2, 4, 6), [[b0], [b1]], w_in, w_out, acc, cols, stored=(0, 2, 4, 6))
    add_rows(0, (0, 1), (0, 1), [[a0, a1]], w_in, w_out, acc, cols, stored=(1,))


def near_kernel(side, *refs):
    own, other, (w_in, w_out), (acc, cols) = refs[0:4], refs[4:8], refs[8:10], refs[-2:]
    b10, b11, b30, b31 = sides(own, other)[side]
    if side == 0:
        rows, blocks = (2, 3, 6, 7), [[b10, b11], [b30, b31]]
    else:
        rows, blocks = (1, 3, 5, 7), [[b10, b30], [b11, b31]]
    add_rows(side, (0, 1), rows, blocks, w_in, w_out, acc, cols)


def far_rows(cut, own, other, w_in, w_out, acc, cols):
    (a0, a1), (b0, b1) = sides(own, other)
    add_rows(0, (0, 1), (4, 5), [[a0, a1]], w_in, w_out, acc, cols, cuts=(CUTS[cut],))
    add_rows(1, (1,), (0, 2, 4, 6), [[b0], [b1]], w_in, w_out, acc, cols, cuts=(CUTS[cut],))


STATE = (jax.ShapeDtypeStruct((3, 8, 128, 640), F32), jax.ShapeDtypeStruct((2, 8, 128, 256), BF16))


def priced(giga):
    return pl.CostEstimate(flops=giga << 30, bytes_accessed=1 << 20, transcendentals=0)


def gathered(kernel, blocks, w_in, w_out, state):
    n = len(blocks)
    return pl.pallas_call(
        kernel,
        out_shape=STATE,
        in_specs=[VMEM] * (n + 2 + len(state)),
        out_specs=(VMEM, VMEM),
        input_output_aliases={n + 2: 0, n + 3: 1} if state else {},
        compiler_params=PARAMS,
        cost_estimate=priced(n // 2),
    )(*blocks, w_in, w_out, *state)


def finished(cut, blocks, w_in, w_out, state, terms):
    width = CUTS[cut][1] - CUTS[cut][0]

    def kernel(*refs):
        own, other, weights, terms = refs[:2], refs[2:4], refs[4:6], refs[8:12]
        acc, cols, *rest = refs[12:]
        far_rows(cut, own, other, *weights, acc, None if cut else cols)
        last_kernel(CUTS[cut], terms, acc, cols, *rest)

    *state, keep, send = pl.pallas_call(
        kernel,
        out_shape=STATE
        + (jax.ShapeDtypeStruct((4, 3, 32, width), F32), jax.ShapeDtypeStruct((4, 3, 32, width), BF16)),
        in_specs=[VMEM] * 12,
        out_specs=(VMEM,) * 4,
        input_output_aliases={6: 0, 7: 1},
        scratch_shapes=[
            pltpu.VMEM((8, 128, 2 * width), BF16),
            pltpu.VMEM((8, 128, width), BF16),
            pltpu.VMEM((8, 3, 32, width), F32),
        ],
        compiler_params=PARAMS,
        cost_estimate=priced(2),
    )(*blocks, w_in, w_out, *state, *terms)
    return state, keep, send


def last_kernel(cut, terms, acc, cols, keep, send, gates, hidden, total):
    xl, y, z, _, c = place()
    lane = lax.broadcasted_iota(I32, (8, 128), 1)
    lower, upper = cut
    width = upper - lower
    row = lax.broadcasted_iota(I32, (8, 128), 0)
    known = (lane < 5) & (row < 4)
    workers = [(((xl ^ ex) * 4 + (y ^ row)) & 7) * 8 + ((z - lane) & 7) for ex in range(2)]

    def part(p, _):
        dy, ex = p >> 1, p & 1
        number = ((xl ^ ex) * 4 + (y ^ dy)) * 8 + z
        w = F32(0.0)
        for i, worker in enumerate(workers):
            mine = known & (((number - lane) & 63) == worker)
            w = w + jnp.sum(jnp.where(mine, terms[2 * i][...] + terms[2 * i + 1][...], 0.0))
        for r in range(0, 128, 32):
            rows = pl.ds(r, 32)
            u = acc[0, p, rows, lower:upper]
            v = acc[1, p, rows, lower:upper]
            d = acc[2, p, rows, lower:upper] * w
            square = u * u
            t = jnp.tanh(ROOT_2_PI * (u + CUBIC * (square * u)))
            cdf = 0.5 * (1.0 + t)
            act = u * cdf
            slope = cdf + 0.5 * u * (1.0 - t * t) * (ROOT_2_PI * (1.0 + 3.0 * CUBIC * square))
            gates[p, rows, :width] = (d * v * slope).astype(BF16)
            gates[p, rows, width:] = (d * act).astype(BF16)
            hidden[p, rows] = (act * v * w).astype(BF16)
        return 0

    lax.fori_loop(0, 8, part, 0)
    dims = (((0,), (0,)), ((), ()))
    both = lax.dot_general(
        cols[0].reshape(1024, 256), gates[...].reshape(1024, 2 * width), dims, preferred_element_type=F32
    )
    total[:, 0] = both[:, :width].reshape(8, 32, width)
    total[:, 1] = both[:, width:].reshape(8, 32, width)
    total[:, 2] = lax.dot_general(
        cols[1].reshape(1024, 256), hidden[...].reshape(1024, width), dims, preferred_element_type=F32
    ).reshape(8, 32, width)
    odd = z & 1
    near = jnp.where(odd == 1, z + 1, z - 1) & 7
    near = jnp.where(c == 0, z ^ 1, near)
    for k in range(4):
        keep[k] = total[((z >> 1) + k & 3) * 2 + odd]
        send[k] = total[((near >> 1) + k & 3) * 2 + (1 - odd)].astype(BF16)


def all_steps(tokens, grad_out, w_gate, w_lin, w_out_t, code, decode, stragglers):
    own = message(code, decode, stragglers, tokens, grad_out)
    first = {}
    for k in (1, 2, 3):
        first[k] = across(own, k, True)
    w_in, w_out = loaded_weights(w_gate, w_lin, w_out_t)
    blocks = {(0, 0): jnp.stack([own, first[1]]), (0, 1): jnp.stack([first[2], first[3]])}
    others = {}
    for k, j in EARLY + LATE:
        blocks[k, j] = across(blocks[0, j], k, False)
    for j, came in ((0, 1), (1, 3)):
        blocks[2, j] = across(blocks[came, j], came ^ 2, False)
    for k, j in OWN + EARLY + LATE:
        others[k, j] = sibling(blocks[k, j])
    rows = line_rows(blocks[0, 0], blocks[0, 1], others[0, 0], others[0, 1])
    got = []
    for j in (1, 3):
        got.append(z_shift(rows, j))
    partial = part_of_line(rows, *got)
    partials = [partial, swapped(partial, "xl", 2, 1)]
    terms = []
    for part in partials:
        terms += [part, sibling(part)]

    def both(keys):
        return [blocks[key] for key in keys] + [others[key] for key in keys]

    state = gathered(first_kernel, both(OWN), w_in, w_out, ())
    pairs = both(sorted(EARLY + LATE))
    state = gathered(partial_call(near_kernel, 0), pairs, w_in, w_out, state)
    state, blocks[2, 0], blocks[2, 1] = lax.optimization_barrier((state, blocks[2, 0], blocks[2, 1]))
    for k, j in FAR:
        others[k, j] = sibling(blocks[k, j])
    state = gathered(partial_call(near_kernel, 1), pairs, w_in, w_out, state)
    halves = both(FAR)
    keeps, got = [], []
    for cut in range(2):
        state, keep, send = finished(cut, halves, w_in, w_out, state, terms)
        keeps.append(keep)
        got.append(z_pair(send))
    results, across_ring = [], []
    for cut in range(2):
        mixed = keeps[cut] + got[cut].astype(F32)
        sends = mixed.astype(BF16)
        if cut == 0:
            sends, keeps[1] = lax.optimization_barrier((sends, keeps[1]))
        across_ring.append(sends[2])
        result = mixed[0]
        for k in (1, 3):
            result = result + z_step(sends[k], 2 * k).astype(F32)
        results.append(result)
    opposite = z_step(jnp.concatenate(across_ring, axis=2), 4)
    return jnp.transpose(jnp.concatenate(results, axis=2) + opposite.astype(F32), (1, 0, 2))


def solution(mesh):
    split = Mesh(mesh.devices.reshape(2, 4, 8, 2, 2), ("xl", "y", "z", "xh", "c"))
    mp = ("xh", "c")
    in_specs = (P(BLK, mp), P(BLK, mp), P(None, mp), P(None, mp), P(None, mp), P(BLK, None), P(BLK), P())
    return jax.shard_map(all_steps, mesh=split, in_specs=in_specs, out_specs=P(BLK, None, mp), check_vma=False)
```

```python
from functools import partial as partial_call

import jax
import jax.numpy as jnp
from jax import lax
from jax.experimental import pallas as pl
from jax.experimental.pallas import tpu as pltpu
from jax.sharding import Mesh, PartitionSpec as P


BF16 = jnp.bfloat16
F32 = jnp.float32
I32 = jnp.int32
ROOT_2_PI = 0.7978845608028654
CUBIC = 0.044715
CUTS = ((0, 384), (384, 640))
OWN, EARLY, LATE, FAR = ((0, 0), (0, 1)), ((1, 0), (3, 1)), ((1, 1), (3, 0)), ((2, 0), (2, 1))
BLK = ("xl", "y", "z")
PLANE = ("xl", "y", "xh", "c")
SMEM = pl.BlockSpec(memory_space=pltpu.SMEM)
VMEM = pl.BlockSpec(memory_space=pltpu.VMEM)
PARAMS = pltpu.CompilerParams(vmem_limit_bytes=16 * 1024 * 1024)


def place():
    return [lax.axis_index(a).astype(I32) for a in ("xl", "y", "z", "xh", "c")]


def across(block, flip, first):
    route = []
    for xl in range(2):
        for y in range(4):
            for xh in range(2):
                for c in range(2):
                    on_x = (c == 0) == first
                    to = (xl ^ (flip & 1), y, xh ^ (flip >> 1), c) if on_x else (xl, y ^ flip, xh, c)
                    number = lambda a: ((a[0] * 4 + a[1]) * 2 + a[2]) * 2 + a[3]
                    route.append((number((xl, y, xh, c)), number(to)))
    return lax.ppermute(block, PLANE, route)


def swapped(block, axis, size, flip):
    return lax.ppermute(block, axis, [(i, i ^ flip) for i in range(size)])


def sibling(block):
    return lax.ppermute(block, "c", [(0, 1), (1, 0)])


def partner_of(z, c):
    return z ^ 1 if c == 0 else ((z + 1) % 8 if z % 2 else (z - 1) % 8)


def z_pair(block):
    return lax.ppermute(block, ("z", "c"), [(z * 2 + c, partner_of(z, c) * 2 + c) for z in range(8) for c in range(2)])


def z_shift(block, step):
    return lax.ppermute(
        block, ("z", "c"), [(z * 2 + c, (z + step + c) % 8 * 2 + c) for z in range(8) for c in range(2)]
    )


def z_step(block, step):
    return lax.ppermute(block, "z", [(z, (z + step) % 8) for z in range(8)])


def hbm(array):
    return pltpu.with_memory_space_constraint(array, pltpu.HBM)


def message_kernel(decode, code_in, stragglers_in, tokens, grad_out, out, code, stragglers, sems):
    pairs = (
        (tokens, out.at[pl.ds(0, 128)]),
        (grad_out, out.at[pl.ds(128, 128)]),
        (code_in, code),
        (stragglers_in, stragglers),
    )
    copies = [pltpu.make_async_copy(source, target, sems.at[i]) for i, (source, target) in enumerate(pairs)]
    for copy in copies:
        copy.start()
    for copy in copies[2:]:
        copy.wait()
    xl, y, z, _, _ = place()
    device = (xl * 4 + y) * 8 + z
    alive = stragglers[0] != device
    for i in range(1, 4):
        alive = alive & (stragglers[i] != device)
    scale = jnp.where(alive, decode[0], 0.0)
    lane = lax.broadcasted_iota(I32, (8, 128), 1)
    row = lax.broadcasted_iota(I32, (8, 128), 0)
    value = jnp.zeros((8, 128), F32)
    for j in range(5):
        value = jnp.where(lane == j, scale * code[0, j], value)
    high = value.astype(BF16).astype(F32)
    rest = value - high
    middle = rest.astype(BF16).astype(F32)
    low = rest - middle
    pieces = jnp.where(row == 0, high, jnp.where(row == 1, middle, jnp.where(row == 2, low, 0.0)))
    out[256:264, :] = jnp.zeros((8, 512), BF16)
    out[256:264, 0:128] = pieces.astype(BF16)
    for copy in copies[:2]:
        copy.wait()


def message(code, decode, stragglers, tokens, grad_out):
    return pl.pallas_call(
        message_kernel,
        out_shape=jax.ShapeDtypeStruct((264, 512), BF16),
        in_specs=[SMEM] + [pl.BlockSpec(memory_space=pltpu.HBM)] * 4,
        out_specs=VMEM,
        scratch_shapes=[pltpu.SMEM((1, 5), F32), pltpu.SMEM((4,), I32), pltpu.SemaphoreType.DMA((4,))],
        compiler_params=PARAMS,
        name="message",
    )(decode, *[hbm(a) for a in (code, stragglers, tokens, grad_out)])


def weights_kernel(w_gate, w_lin, w_out_t, w_in, w_out, sems):
    xh = lax.axis_index("xh").astype(I32)
    copies = []
    for side in range(2):
        for eh in range(2):
            source, target = 2 * (xh ^ eh) + side, pl.ds(512 * (2 * side + eh), 512)
            copies.append((w_out_t.at[source], w_out.at[target]))
            for lower, upper in CUTS:
                width = upper - lower
                for n, w in enumerate((w_gate, w_lin)):
                    columns = pl.ds(2 * lower + n * width, width)
                    copies.append((w.at[source, :, pl.ds(lower, width)], w_in.at[target, columns]))
    copies = [pltpu.make_async_copy(*pair, sems.at[i]) for i, pair in enumerate(copies)]
    for copy in copies:
        copy.start()
    for copy in copies:
        copy.wait()


def loaded_weights(w_gate, w_lin, w_out_t):
    return pl.pallas_call(
        weights_kernel,
        out_shape=(
            jax.ShapeDtypeStruct((2048, 1280), BF16),
            jax.ShapeDtypeStruct((2048, 640), BF16),
        ),
        in_specs=[pl.BlockSpec(memory_space=pltpu.HBM)] * 3,
        out_specs=(VMEM, VMEM),
        scratch_shapes=[pltpu.SemaphoreType.DMA((20,))],
        compiler_params=PARAMS,
        name="load",
    )(*[hbm(w.reshape(4, 512, 640)) for w in (w_gate, w_lin, w_out_t)])


def rows_kernel(own_low, own_high, other_low, other_high, rows):
    c = lax.axis_index("c").astype(I32)
    rows[...] = jnp.zeros_like(rows)
    for dy in range(4):
        pair = (own_low, other_low) if dy < 2 else (own_high, other_high)
        piece = [block[dy % 2, 256:264, 0:128].astype(F32) for block in pair]
        piece = jnp.where(c == 1, piece[0], piece[1])
        rows[dy : dy + 1, :] = jnp.sum(piece, axis=0, keepdims=True)


def line_rows(*blocks):
    return pl.pallas_call(
        rows_kernel,
        out_shape=jax.ShapeDtypeStruct((8, 128), F32),
        in_specs=[VMEM] * 4,
        out_specs=VMEM,
        compiler_params=PARAMS,
        name="rows",
    )(*blocks)


def part_kernel(rows, near, far, out):
    c = lax.axis_index("c").astype(I32)
    lane = lax.broadcasted_iota(I32, (8, 128), 1)
    total = jnp.where((lane == 0) & (c == 0), rows[...], 0.0)
    total = jnp.where(lane == 1 + c, near[...], total)
    out[...] = jnp.where(lane == 3 + c, far[...], total)


def part_of_line(*rows):
    return pl.pallas_call(
        part_kernel,
        out_shape=jax.ShapeDtypeStruct((8, 128), F32),
        in_specs=[VMEM] * 3,
        out_specs=VMEM,
        compiler_params=PARAMS,
        name="part",
    )(*rows)


def sides(own, other):
    c = lax.axis_index("c").astype(I32)
    pairs = [(mine[...], theirs[...]) for mine, theirs in zip(own, other)]
    x_first = [jnp.where(c == 0, mine, theirs) for mine, theirs in pairs]
    y_first = [jnp.where(c == 0, theirs, mine) for mine, theirs in pairs]
    return x_first, y_first


def add_rows(side, ehs, rows, blocks, w_in, w_out, acc, cols, stored=(), cuts=CUTS):
    xl, y, _, xh, _ = place()
    low, end = 1024 * side + 512 * ehs[0], 1024 * side + 512 * (ehs[-1] + 1)
    parts = []
    for n in range(2):
        pieces = [[b[:, 128 * n : 128 * n + 128].reshape(256, 512) for b in row] for row in blocks]
        parts.append(jnp.concatenate([jnp.concatenate(p, axis=1) for p in pieces], axis=0))
    first, last = cuts[0][0], cuts[-1][1]
    pre = jnp.dot(parts[0], w_in[low:end, 2 * first : 2 * last], preferred_element_type=F32)
    dh = jnp.dot(parts[1], w_out[low:end, first:last], preferred_element_type=F32)
    for i, p in enumerate(rows):
        at_rows = slice(128 * i, 128 * i + 128)
        values = [(2, first, last, dh[at_rows])]
        for lower, upper in cuts:
            for n in range(2):
                at = 2 * (lower - first) + n * (upper - lower)
                values.append((n, lower, upper, pre[at_rows, at : at + upper - lower]))
        for n, lower, upper, value in values:
            if p in stored:
                acc[n, p, :, lower:upper] = value
            else:
                acc[n, p, :, lower:upper] += value
    if cols is None:
        return
    for k, eh in enumerate(ehs):

        @pl.when(((y >> 1) == side) & ((xl ^ xh) == eh))
        def _():
            for n in range(2):
                v = parts[n][:, 512 * k : 512 * k + 512]
                v = jnp.where((y & 1) == 0, v[:, :256], v[:, 256:])
                for i, p in enumerate(rows):
                    cols[n, p] = v[128 * i : 128 * i + 128]


def first_kernel(own0, own1, other0, other1, w_in, w_out, acc, cols):
    (a0, a1), (b0, b1) = sides((own0, own1), (other0, other1))
    for p in (3, 5, 7):
        acc[:, p] = jnp.zeros((3, 128, 640), F32)
    add_rows(1, (0,), (0, 2, 4, 6), [[b0], [b1]], w_in, w_out, acc, cols, stored=(0, 2, 4, 6))
    add_rows(0, (0, 1), (0, 1), [[a0, a1]], w_in, w_out, acc, cols, stored=(1,))


def near_kernel(side, *refs):
    own, other, (w_in, w_out), (acc, cols) = refs[0:4], refs[4:8], refs[8:10], refs[-2:]
    b10, b11, b30, b31 = sides(own, other)[side]
    if side == 0:
        rows, blocks = (2, 3, 6, 7), [[b10, b11], [b30, b31]]
    else:
        rows, blocks = (1, 3, 5, 7), [[b10, b30], [b11, b31]]
    add_rows(side, (0, 1), rows, blocks, w_in, w_out, acc, cols)


def far_rows(cut, own, other, w_in, w_out, acc, cols):
    (a0, a1), (b0, b1) = sides(own, other)
    add_rows(0, (0, 1), (4, 5), [[a0, a1]], w_in, w_out, acc, cols, cuts=(CUTS[cut],))
    add_rows(1, (1,), (0, 2, 4, 6), [[b0], [b1]], w_in, w_out, acc, cols, cuts=(CUTS[cut],))


STATE = (jax.ShapeDtypeStruct((3, 8, 128, 640), F32), jax.ShapeDtypeStruct((2, 8, 128, 256), BF16))


def priced(giga):
    return pl.CostEstimate(flops=giga << 30, bytes_accessed=1 << 20, transcendentals=0)


def gathered(kernel, blocks, w_in, w_out, state):
    n = len(blocks)
    return pl.pallas_call(
        kernel,
        out_shape=STATE,
        in_specs=[VMEM] * (n + 2 + len(state)),
        out_specs=(VMEM, VMEM),
        input_output_aliases={n + 2: 0, n + 3: 1} if state else {},
        compiler_params=PARAMS,
        cost_estimate=priced(n // 2),
    )(*blocks, w_in, w_out, *state)


def finished(cut, blocks, w_in, w_out, state, terms):
    width = CUTS[cut][1] - CUTS[cut][0]

    def kernel(*refs):
        own, other, weights, terms = refs[:2], refs[2:4], refs[4:6], refs[8:12]
        acc, cols, *rest = refs[12:]
        far_rows(cut, own, other, *weights, acc, None if cut else cols)
        last_kernel(CUTS[cut], terms, acc, cols, *rest)

    *state, keep, send = pl.pallas_call(
        kernel,
        out_shape=STATE
        + (jax.ShapeDtypeStruct((4, 3, 32, width), F32), jax.ShapeDtypeStruct((4, 3, 32, width), BF16)),
        in_specs=[VMEM] * 12,
        out_specs=(VMEM,) * 4,
        input_output_aliases={6: 0, 7: 1},
        scratch_shapes=[
            pltpu.VMEM((8, 128, 2 * width), BF16),
            pltpu.VMEM((8, 128, width), BF16),
            pltpu.VMEM((8, 3, 32, width), F32),
        ],
        compiler_params=PARAMS,
        cost_estimate=priced(2),
    )(*blocks, w_in, w_out, *state, *terms)
    return state, keep, send


def last_kernel(cut, terms, acc, cols, keep, send, gates, hidden, total):
    xl, y, z, _, c = place()
    lane = lax.broadcasted_iota(I32, (8, 128), 1)
    lower, upper = cut
    width = upper - lower
    row = lax.broadcasted_iota(I32, (8, 128), 0)
    known = (lane < 5) & (row < 4)
    workers = [(((xl ^ ex) * 4 + (y ^ row)) & 7) * 8 + ((z - lane) & 7) for ex in range(2)]

    def part(p, _):
        dy, ex = p >> 1, p & 1
        number = ((xl ^ ex) * 4 + (y ^ dy)) * 8 + z
        w = F32(0.0)
        for i, worker in enumerate(workers):
            mine = known & (((number - lane) & 63) == worker)
            w = w + jnp.sum(jnp.where(mine, terms[2 * i][...] + terms[2 * i + 1][...], 0.0))
        for r in range(0, 128, 32):
            rows = pl.ds(r, 32)
            u = acc[0, p, rows, lower:upper]
            v = acc[1, p, rows, lower:upper]
            d = acc[2, p, rows, lower:upper] * w
            square = u * u
            t = jnp.tanh(ROOT_2_PI * (u + CUBIC * (square * u)))
            cdf = 0.5 * (1.0 + t)
            act = u * cdf
            slope = cdf + 0.5 * u * (1.0 - t * t) * (ROOT_2_PI * (1.0 + 3.0 * CUBIC * square))
            gates[p, rows, :width] = (d * v * slope).astype(BF16)
            gates[p, rows, width:] = (d * act).astype(BF16)
            hidden[p, rows] = (act * v * w).astype(BF16)
        return 0

    lax.fori_loop(0, 8, part, 0)
    dims = (((0,), (0,)), ((), ()))
    both = lax.dot_general(
        cols[0].reshape(1024, 256), gates[...].reshape(1024, 2 * width), dims, preferred_element_type=F32
    )
    total[:, 0] = both[:, :width].reshape(8, 32, width)
    total[:, 1] = both[:, width:].reshape(8, 32, width)
    total[:, 2] = lax.dot_general(
        cols[1].reshape(1024, 256), hidden[...].reshape(1024, width), dims, preferred_element_type=F32
    ).reshape(8, 32, width)
    odd = z & 1
    near = jnp.where(odd == 1, z + 1, z - 1) & 7
    near = jnp.where(c == 0, z ^ 1, near)
    for k in range(4):
        keep[k] = total[((z >> 1) + k & 3) * 2 + odd]
        send[k] = total[((near >> 1) + k & 3) * 2 + (1 - odd)].astype(BF16)


def mix_kernel(keep, got, *refs):
    mixed = [keep[k] + got[k].astype(F32) for k in range(4)]
    width = keep.shape[-1]
    if len(refs) == 5:
        before, own, plus, minus, opposite = refs
        opposite[:, :, : 640 - width] = before[...]
        opposite[:, :, 640 - width :] = mixed[2].astype(BF16)
    else:
        own, plus, minus, opposite = refs
        opposite[...] = mixed[2].astype(BF16)
    own[...] = mixed[0]
    plus[...] = mixed[1].astype(BF16)
    minus[...] = mixed[3].astype(BF16)


def mixed(keep, got, *before):
    width = keep.shape[-1]
    shape = (3, 32, width)
    return pl.pallas_call(
        mix_kernel,
        out_shape=(
            jax.ShapeDtypeStruct(shape, F32),
            jax.ShapeDtypeStruct(shape, BF16),
            jax.ShapeDtypeStruct(shape, BF16),
            jax.ShapeDtypeStruct((3, 32, 640) if before else shape, BF16),
        ),
        in_specs=[VMEM] * (2 + len(before)),
        out_specs=(VMEM,) * 4,
        compiler_params=PARAMS,
    )(keep, got, *before)


def all_steps(tokens, grad_out, w_gate, w_lin, w_out_t, code, decode, stragglers):
    own = message(code, decode, stragglers, tokens, grad_out)
    first = {}
    for k in (1, 2, 3):
        first[k] = across(own, k, True)
    w_in, w_out = loaded_weights(w_gate, w_lin, w_out_t)
    blocks = {(0, 0): jnp.stack([own, first[1]]), (0, 1): jnp.stack([first[2], first[3]])}
    others = {}
    for k, j in EARLY + LATE:
        blocks[k, j] = across(blocks[0, j], k, False)
    for j, came in ((0, 1), (1, 3)):
        blocks[2, j] = across(blocks[came, j], came ^ 2, False)
    for k, j in OWN + EARLY + LATE:
        others[k, j] = sibling(blocks[k, j])
    rows = line_rows(blocks[0, 0], blocks[0, 1], others[0, 0], others[0, 1])
    got = []
    for j in (1, 3):
        got.append(z_shift(rows, j))
    partial = part_of_line(rows, *got)
    partials = [partial, swapped(partial, "xl", 2, 1)]
    terms = []
    for part in partials:
        terms += [part, sibling(part)]

    def both(keys):
        return [blocks[key] for key in keys] + [others[key] for key in keys]

    state = gathered(first_kernel, both(OWN), w_in, w_out, ())
    pairs = both(sorted(EARLY + LATE))
    state = gathered(partial_call(near_kernel, 0), pairs, w_in, w_out, state)
    state, blocks[2, 0], blocks[2, 1] = lax.optimization_barrier((state, blocks[2, 0], blocks[2, 1]))
    for k, j in FAR:
        others[k, j] = sibling(blocks[k, j])
    state = gathered(partial_call(near_kernel, 1), pairs, w_in, w_out, state)
    halves = both(FAR)
    keeps, got = [], []
    for cut in range(2):
        state, keep, send = finished(cut, halves, w_in, w_out, state, terms)
        keeps.append(keep)
        got.append(z_pair(send))
    results, opposite = [], []
    for cut in range(2):
        own, plus, minus, opposite = mixed(keeps[cut], got[cut], *([opposite] if cut else []))
        result = own
        for k, block in ((1, plus), (3, minus)):
            result = result + z_step(block, 2 * k).astype(F32)
        results.append(result)
    opposite = z_step(opposite, 4)
    return jnp.transpose(jnp.concatenate(results, axis=2) + opposite.astype(F32), (1, 0, 2))


def solution(mesh):
    split = Mesh(mesh.devices.reshape(2, 4, 8, 2, 2), ("xl", "y", "z", "xh", "c"))
    mp = ("xh", "c")
    in_specs = (P(BLK, mp), P(BLK, mp), P(None, mp), P(None, mp), P(None, mp), P(BLK, None), P(BLK), P())
    return jax.shard_map(all_steps, mesh=split, in_specs=in_specs, out_specs=P(BLK, None, mp), check_vma=False)
```

```python
from functools import partial as partial_call

import jax
import jax.numpy as jnp
from jax import lax
from jax.experimental import pallas as pl
from jax.experimental.pallas import tpu as pltpu
from jax.sharding import Mesh, PartitionSpec as P


BF16 = jnp.bfloat16
F32 = jnp.float32
I32 = jnp.int32
ROOT_2_PI = 0.7978845608028654
CUBIC = 0.044715
CUTS = ((0, 384), (384, 640))
OWN, EARLY, LATE, FAR = ((0, 0), (0, 1)), ((1, 0), (3, 1)), ((1, 1), (3, 0)), ((2, 0), (2, 1))
BLK = ("xl", "y", "z")
PLANE = ("xl", "y", "xh", "c")
SMEM = pl.BlockSpec(memory_space=pltpu.SMEM)
VMEM = pl.BlockSpec(memory_space=pltpu.VMEM)
PARAMS = pltpu.CompilerParams(vmem_limit_bytes=16 * 1024 * 1024)


def place():
    return [lax.axis_index(a).astype(I32) for a in ("xl", "y", "z", "xh", "c")]


def across(block, flip, first):
    route = []
    for xl in range(2):
        for y in range(4):
            for xh in range(2):
                for c in range(2):
                    on_x = (c == 0) == first
                    to = (xl ^ (flip & 1), y, xh ^ (flip >> 1), c) if on_x else (xl, y ^ flip, xh, c)
                    number = lambda a: ((a[0] * 4 + a[1]) * 2 + a[2]) * 2 + a[3]
                    route.append((number((xl, y, xh, c)), number(to)))
    return lax.ppermute(block, PLANE, route)


def swapped(block, axis, size, flip):
    return lax.ppermute(block, axis, [(i, i ^ flip) for i in range(size)])


def sibling(block):
    return lax.ppermute(block, "c", [(0, 1), (1, 0)])


def partner_of(z, c):
    return z ^ 1 if c == 0 else ((z + 1) % 8 if z % 2 else (z - 1) % 8)


def z_pair(block):
    return lax.ppermute(block, ("z", "c"), [(z * 2 + c, partner_of(z, c) * 2 + c) for z in range(8) for c in range(2)])


def z_shift(block, step):
    return lax.ppermute(
        block, ("z", "c"), [(z * 2 + c, (z + step + c) % 8 * 2 + c) for z in range(8) for c in range(2)]
    )


def z_step(block, step):
    return lax.ppermute(block, "z", [(z, (z + step) % 8) for z in range(8)])


def hbm(array):
    return pltpu.with_memory_space_constraint(array, pltpu.HBM)


def message_kernel(decode, code_in, stragglers_in, tokens, grad_out, out, code, stragglers, sems):
    pairs = (
        (tokens, out.at[pl.ds(0, 128)]),
        (grad_out, out.at[pl.ds(128, 128)]),
        (code_in, code),
        (stragglers_in, stragglers),
    )
    copies = [pltpu.make_async_copy(source, target, sems.at[i]) for i, (source, target) in enumerate(pairs)]
    for copy in copies:
        copy.start()
    for copy in copies[2:]:
        copy.wait()
    xl, y, z, _, _ = place()
    device = (xl * 4 + y) * 8 + z
    alive = stragglers[0] != device
    for i in range(1, 4):
        alive = alive & (stragglers[i] != device)
    scale = jnp.where(alive, decode[0], 0.0)
    lane = lax.broadcasted_iota(I32, (8, 128), 1)
    row = lax.broadcasted_iota(I32, (8, 128), 0)
    value = jnp.zeros((8, 128), F32)
    for j in range(5):
        value = jnp.where(lane == j, scale * code[0, j], value)
    high = value.astype(BF16).astype(F32)
    rest = value - high
    middle = rest.astype(BF16).astype(F32)
    low = rest - middle
    pieces = jnp.where(row == 0, high, jnp.where(row == 1, middle, jnp.where(row == 2, low, 0.0)))
    out[256:264, :] = jnp.zeros((8, 512), BF16)
    out[256:264, 0:128] = pieces.astype(BF16)
    for copy in copies[:2]:
        copy.wait()


def message(code, decode, stragglers, tokens, grad_out):
    return pl.pallas_call(
        message_kernel,
        out_shape=jax.ShapeDtypeStruct((264, 512), BF16),
        in_specs=[SMEM] + [pl.BlockSpec(memory_space=pltpu.HBM)] * 4,
        out_specs=VMEM,
        scratch_shapes=[pltpu.SMEM((1, 5), F32), pltpu.SMEM((4,), I32), pltpu.SemaphoreType.DMA((4,))],
        compiler_params=PARAMS,
        name="message",
    )(decode, *[hbm(a) for a in (code, stragglers, tokens, grad_out)])


def weights_kernel(w_gate, w_lin, w_out_t, w_in, w_out, sems):
    xh = lax.axis_index("xh").astype(I32)
    copies = []
    for side in range(2):
        for eh in range(2):
            source, target = 2 * (xh ^ eh) + side, pl.ds(512 * (2 * side + eh), 512)
            copies.append((w_out_t.at[source], w_out.at[target]))
            for lower, upper in CUTS:
                width = upper - lower
                for n, w in enumerate((w_gate, w_lin)):
                    columns = pl.ds(2 * lower + n * width, width)
                    copies.append((w.at[source, :, pl.ds(lower, width)], w_in.at[target, columns]))
    copies = [pltpu.make_async_copy(*pair, sems.at[i]) for i, pair in enumerate(copies)]
    for copy in copies:
        copy.start()
    for copy in copies:
        copy.wait()


def loaded_weights(w_gate, w_lin, w_out_t):
    return pl.pallas_call(
        weights_kernel,
        out_shape=(
            jax.ShapeDtypeStruct((2048, 1280), BF16),
            jax.ShapeDtypeStruct((2048, 640), BF16),
        ),
        in_specs=[pl.BlockSpec(memory_space=pltpu.HBM)] * 3,
        out_specs=(VMEM, VMEM),
        scratch_shapes=[pltpu.SemaphoreType.DMA((20,))],
        compiler_params=PARAMS,
        name="load",
    )(*[hbm(w.reshape(4, 512, 640)) for w in (w_gate, w_lin, w_out_t)])


def rows_kernel(own_low, own_high, other_low, other_high, rows):
    c = lax.axis_index("c").astype(I32)
    rows[...] = jnp.zeros_like(rows)
    for dy in range(4):
        pair = (own_low, other_low) if dy < 2 else (own_high, other_high)
        piece = [block[dy % 2, 256:264, 0:128].astype(F32) for block in pair]
        piece = jnp.where(c == 1, piece[0], piece[1])
        rows[dy : dy + 1, :] = jnp.sum(piece, axis=0, keepdims=True)


def line_rows(*blocks):
    return pl.pallas_call(
        rows_kernel,
        out_shape=jax.ShapeDtypeStruct((8, 128), F32),
        in_specs=[VMEM] * 4,
        out_specs=VMEM,
        compiler_params=PARAMS,
        name="rows",
    )(*blocks)


def part_kernel(rows, near, far, out):
    c = lax.axis_index("c").astype(I32)
    lane = lax.broadcasted_iota(I32, (8, 128), 1)
    total = jnp.where((lane == 0) & (c == 0), rows[...], 0.0)
    total = jnp.where(lane == 1 + c, near[...], total)
    out[...] = jnp.where(lane == 3 + c, far[...], total)


def part_of_line(*rows):
    return pl.pallas_call(
        part_kernel,
        out_shape=jax.ShapeDtypeStruct((8, 128), F32),
        in_specs=[VMEM] * 3,
        out_specs=VMEM,
        compiler_params=PARAMS,
        name="part",
    )(*rows)


def sides(own, other):
    c = lax.axis_index("c").astype(I32)
    pairs = [(mine[...], theirs[...]) for mine, theirs in zip(own, other)]
    x_first = [jnp.where(c == 0, mine, theirs) for mine, theirs in pairs]
    y_first = [jnp.where(c == 0, theirs, mine) for mine, theirs in pairs]
    return x_first, y_first


def add_rows(side, ehs, rows, blocks, w_in, w_out, acc, cols, stored=(), cuts=CUTS):
    xl, y, _, xh, _ = place()
    low, end = 1024 * side + 512 * ehs[0], 1024 * side + 512 * (ehs[-1] + 1)
    parts = []
    for n in range(2):
        pieces = [[b[:, 128 * n : 128 * n + 128].reshape(256, 512) for b in row] for row in blocks]
        parts.append(jnp.concatenate([jnp.concatenate(p, axis=1) for p in pieces], axis=0))
    first, last = cuts[0][0], cuts[-1][1]
    pre = jnp.dot(parts[0], w_in[low:end, 2 * first : 2 * last], preferred_element_type=F32)
    dh = jnp.dot(parts[1], w_out[low:end, first:last], preferred_element_type=F32)
    for i, p in enumerate(rows):
        at_rows = slice(128 * i, 128 * i + 128)
        values = [(2, first, last, dh[at_rows])]
        for lower, upper in cuts:
            for n in range(2):
                at = 2 * (lower - first) + n * (upper - lower)
                values.append((n, lower, upper, pre[at_rows, at : at + upper - lower]))
        for n, lower, upper, value in values:
            if p in stored:
                acc[n, p, :, lower:upper] = value
            else:
                acc[n, p, :, lower:upper] += value
    if cols is None:
        return
    for k, eh in enumerate(ehs):

        @pl.when(((y >> 1) == side) & ((xl ^ xh) == eh))
        def _():
            for n in range(2):
                v = parts[n][:, 512 * k : 512 * k + 512]
                v = jnp.where((y & 1) == 0, v[:, :256], v[:, 256:])
                for i, p in enumerate(rows):
                    cols[n, p] = v[128 * i : 128 * i + 128]


def first_kernel(own0, own1, other0, other1, w_in, w_out, acc, cols):
    (a0, a1), (b0, b1) = sides((own0, own1), (other0, other1))
    for p in (3, 5, 7):
        acc[:, p] = jnp.zeros((3, 128, 640), F32)
    add_rows(1, (0,), (0, 2, 4, 6), [[b0], [b1]], w_in, w_out, acc, cols, stored=(0, 2, 4, 6))
    add_rows(0, (0, 1), (0, 1), [[a0, a1]], w_in, w_out, acc, cols, stored=(1,))


def near_kernel(side, *refs):
    own, other, (w_in, w_out), (acc, cols) = refs[0:4], refs[4:8], refs[8:10], refs[-2:]
    b10, b11, b30, b31 = sides(own, other)[side]
    if side == 0:
        rows, blocks = (2, 3, 6, 7), [[b10, b11], [b30, b31]]
    else:
        rows, blocks = (1, 3, 5, 7), [[b10, b30], [b11, b31]]
    add_rows(side, (0, 1), rows, blocks, w_in, w_out, acc, cols)


def far_rows(cut, own, other, w_in, w_out, acc, cols):
    (a0, a1), (b0, b1) = sides(own, other)
    add_rows(0, (0, 1), (4, 5), [[a0, a1]], w_in, w_out, acc, cols, cuts=(CUTS[cut],))
    add_rows(1, (1,), (0, 2, 4, 6), [[b0], [b1]], w_in, w_out, acc, cols, cuts=(CUTS[cut],))


STATE = (jax.ShapeDtypeStruct((3, 8, 128, 640), F32), jax.ShapeDtypeStruct((2, 8, 128, 256), BF16))


def priced(giga):
    return pl.CostEstimate(flops=giga << 30, bytes_accessed=1 << 20, transcendentals=0)


def gathered(kernel, blocks, w_in, w_out, state):
    n = len(blocks)
    return pl.pallas_call(
        kernel,
        out_shape=STATE,
        in_specs=[VMEM] * (n + 2 + len(state)),
        out_specs=(VMEM, VMEM),
        input_output_aliases={n + 2: 0, n + 3: 1} if state else {},
        compiler_params=PARAMS,
        cost_estimate=priced(n // 2),
    )(*blocks, w_in, w_out, *state)


def finished(cut, blocks, w_in, w_out, state, terms):
    width = CUTS[cut][1] - CUTS[cut][0]

    def kernel(*refs):
        own, other, weights, terms = refs[:2], refs[2:4], refs[4:6], refs[8:12]
        acc, cols, *rest = refs[12:]
        far_rows(cut, own, other, *weights, acc, None if cut else cols)
        last_kernel(CUTS[cut], terms, acc, cols, *rest)

    *state, keep, send = pl.pallas_call(
        kernel,
        out_shape=STATE
        + (jax.ShapeDtypeStruct((4, 3, 32, width), F32), jax.ShapeDtypeStruct((4, 3, 32, width), BF16)),
        in_specs=[VMEM] * 12,
        out_specs=(VMEM,) * 4,
        input_output_aliases={6: 0, 7: 1},
        scratch_shapes=[
            pltpu.VMEM((8, 128, 2 * width), BF16),
            pltpu.VMEM((8, 128, width), BF16),
            pltpu.VMEM((8, 3, 32, width), F32),
        ],
        compiler_params=PARAMS,
        cost_estimate=priced(2),
    )(*blocks, w_in, w_out, *state, *terms)
    return state, keep, send


def last_kernel(cut, terms, acc, cols, keep, send, gates, hidden, total):
    xl, y, z, _, c = place()
    lane = lax.broadcasted_iota(I32, (8, 128), 1)
    lower, upper = cut
    width = upper - lower
    row = lax.broadcasted_iota(I32, (8, 128), 0)
    known = (lane < 5) & (row < 4)
    workers = [(((xl ^ ex) * 4 + (y ^ row)) & 7) * 8 + ((z - lane) & 7) for ex in range(2)]

    def part(p, _):
        dy, ex = p >> 1, p & 1
        number = ((xl ^ ex) * 4 + (y ^ dy)) * 8 + z
        w = F32(0.0)
        for i, worker in enumerate(workers):
            mine = known & (((number - lane) & 63) == worker)
            w = w + jnp.sum(jnp.where(mine, terms[2 * i][...] + terms[2 * i + 1][...], 0.0))
        for r in range(0, 128, 32):
            rows = pl.ds(r, 32)
            u = acc[0, p, rows, lower:upper]
            v = acc[1, p, rows, lower:upper]
            d = acc[2, p, rows, lower:upper] * w
            square = u * u
            t = jnp.tanh(u * (ROOT_2_PI + (ROOT_2_PI * CUBIC) * square))
            cdf = 0.5 + 0.5 * t
            act = u * cdf
            slope = cdf + act * (1.0 - t) * (ROOT_2_PI + (3.0 * CUBIC * ROOT_2_PI) * square)
            gates[p, rows, :width] = (d * v * slope).astype(BF16)
            gates[p, rows, width:] = (d * act).astype(BF16)
            hidden[p, rows] = (act * v * w).astype(BF16)
        return 0

    lax.fori_loop(0, 8, part, 0)
    dims = (((0,), (0,)), ((), ()))
    both = lax.dot_general(
        cols[0].reshape(1024, 256), gates[...].reshape(1024, 2 * width), dims, preferred_element_type=F32
    )
    total[:, 0] = both[:, :width].reshape(8, 32, width)
    total[:, 1] = both[:, width:].reshape(8, 32, width)
    total[:, 2] = lax.dot_general(
        cols[1].reshape(1024, 256), hidden[...].reshape(1024, width), dims, preferred_element_type=F32
    ).reshape(8, 32, width)
    odd = z & 1
    near = jnp.where(odd == 1, z + 1, z - 1) & 7
    near = jnp.where(c == 0, z ^ 1, near)
    for k in range(4):
        keep[k] = total[((z >> 1) + k & 3) * 2 + odd]
        send[k] = total[((near >> 1) + k & 3) * 2 + (1 - odd)].astype(BF16)


def mix_kernel(keep, got, *refs):
    mixed = [keep[k] + got[k].astype(F32) for k in range(4)]
    width = keep.shape[-1]
    if len(refs) == 5:
        before, own, plus, minus, opposite = refs
        opposite[:, :, : 640 - width] = before[...]
        opposite[:, :, 640 - width :] = mixed[2].astype(BF16)
    else:
        own, plus, minus, opposite = refs
        opposite[...] = mixed[2].astype(BF16)
    own[...] = mixed[0]
    plus[...] = mixed[1].astype(BF16)
    minus[...] = mixed[3].astype(BF16)


def mixed(keep, got, *before):
    width = keep.shape[-1]
    shape = (3, 32, width)
    return pl.pallas_call(
        mix_kernel,
        out_shape=(
            jax.ShapeDtypeStruct(shape, F32),
            jax.ShapeDtypeStruct(shape, BF16),
            jax.ShapeDtypeStruct(shape, BF16),
            jax.ShapeDtypeStruct((3, 32, 640) if before else shape, BF16),
        ),
        in_specs=[VMEM] * (2 + len(before)),
        out_specs=(VMEM,) * 4,
        compiler_params=PARAMS,
    )(keep, got, *before)


def all_steps(tokens, grad_out, w_gate, w_lin, w_out_t, code, decode, stragglers):
    own = message(code, decode, stragglers, tokens, grad_out)
    first = {}
    for k in (1, 2, 3):
        first[k] = across(own, k, True)
    w_in, w_out = loaded_weights(w_gate, w_lin, w_out_t)
    blocks = {(0, 0): jnp.stack([own, first[1]]), (0, 1): jnp.stack([first[2], first[3]])}
    others = {}
    for k, j in EARLY + LATE:
        blocks[k, j] = across(blocks[0, j], k, False)
    for j, came in ((0, 1), (1, 3)):
        blocks[2, j] = across(blocks[came, j], came ^ 2, False)
    for k, j in OWN + EARLY + LATE:
        others[k, j] = sibling(blocks[k, j])
    rows = line_rows(blocks[0, 0], blocks[0, 1], others[0, 0], others[0, 1])
    got = []
    for j in (1, 3):
        got.append(z_shift(rows, j))
    partial = part_of_line(rows, *got)
    partials = [partial, swapped(partial, "xl", 2, 1)]
    terms = []
    for part in partials:
        terms += [part, sibling(part)]

    def both(keys):
        return [blocks[key] for key in keys] + [others[key] for key in keys]

    state = gathered(first_kernel, both(OWN), w_in, w_out, ())
    pairs = both(sorted(EARLY + LATE))
    state = gathered(partial_call(near_kernel, 0), pairs, w_in, w_out, state)
    state, blocks[2, 0], blocks[2, 1] = lax.optimization_barrier((state, blocks[2, 0], blocks[2, 1]))
    for k, j in FAR:
        others[k, j] = sibling(blocks[k, j])
    state = gathered(partial_call(near_kernel, 1), pairs, w_in, w_out, state)
    halves = both(FAR)
    keeps, got = [], []
    for cut in range(2):
        state, keep, send = finished(cut, halves, w_in, w_out, state, terms)
        keeps.append(keep)
        got.append(z_pair(send))
    results, opposite = [], []
    for cut in range(2):
        own, plus, minus, opposite = mixed(keeps[cut], got[cut], *([opposite] if cut else []))
        result = own
        for k, block in ((1, plus), (3, minus)):
            result = result + z_step(block, 2 * k).astype(F32)
        results.append(result)
    opposite = z_step(opposite, 4)
    return jnp.transpose(jnp.concatenate(results, axis=2) + opposite.astype(F32), (1, 0, 2))


def solution(mesh):
    split = Mesh(mesh.devices.reshape(2, 4, 8, 2, 2), ("xl", "y", "z", "xh", "c"))
    mp = ("xh", "c")
    in_specs = (P(BLK, mp), P(BLK, mp), P(None, mp), P(None, mp), P(None, mp), P(BLK, None), P(BLK), P())
    return jax.shard_map(all_steps, mesh=split, in_specs=in_specs, out_specs=P(BLK, None, mp), check_vma=False)
```
